32 devices in a mesh: facet: 4 (over z), sub: 2 (over x), base: 4 (over y, core).
Axes of the slice: x: 2, y: 2, z: 4, core: 2. Of those that a mesh axis runs over, the one named last changes fastest.
Arguments:
- sky_image: bfloat16 [16384, 1024], P(('facet', 'base')), may hold values from -6 to 6
- facet_rows: int32 [4], replicated, may hold values from 0 to 126976
- column_offset: int32 [1], replicated, may hold values from 0 to 130816
- subgrid_offsets: int32 [2], replicated, may hold values from 0 to 130816
- vis_u: int32 [2, 32768], P('sub', ('facet', 'base')), may hold values from 0 to 1023
- vis_v: int32 [2, 32768], P('sub', ('facet', 'base')), may hold values from 0 to 1023
- observed: float32 [2, 2, 32768], P('sub', None, ('facet', 'base')), may hold values from -6 to 6
- weights: float32 [2, 32768], P('sub', ('facet', 'base')), may hold values from 0.3 to 3
- block_counts: int32 [2, 16], P('sub', ('facet', 'base')), may hold values from 1 to 16
Outputs:
- residual: float32 [2, 2, 32768], P('sub', None, ('facet', 'base'))
- facet_update: bfloat16 [16384, 1024], P(('facet', 'base'), 'sub')
The draws below stay inside these ranges and needn't reach their ends.
Inputs may be any that keep to these rules, and one draw needn't show every extreme that they name: `block_counts`: the live blocks of a shard are its first ones.
All inputs are finite; a program needn't handle non-finite values.
Results may differ from the reference program's by a relative error of at most 0.008.
Values may be sent and summed in bfloat16 or wider, within the bound.
A program may use at most 64 MiB of HBM per device.

```python
import math
import jax
import jax.numpy as jnp
from jax import lax

NIMG = 131072
FS = 4096
CS = 1024
M = 256
SUBW = 1024
BLOCK = 128
VB_DEV = 16
SUBS = 2
ROWS = 16384
VIS = 32768
N_FACET = 4
N_BASE = 4


def place_ends(array, own_key, smallest, high):
    extent = array.shape
    index_at = [jax.random.randint(jax.random.fold_in(own_key, axis), (), 0, extent[axis]) for axis in range(len(extent))]
    array = array.at[tuple(index_at)].set(smallest)
    longest = extent.index(max(extent))
    index_at[longest] = (index_at[longest] + 1) % extent[longest]
    return array.at[tuple(index_at)].set(high)


def shard_levels(stream_key, shape, pieces, least, largest):
    gain, own = 1.0, jax.random.fold_in(stream_key, 6)
    for position, blocks in pieces:
        steps = jnp.exp(jax.random.uniform(jax.random.fold_in(own, position), (blocks,), jnp.float32, least / len(pieces), largest / len(pieces)))
        gain = gain * jnp.repeat(steps, shape[position] // blocks).reshape([-1 if axis == position else 1 for axis in range(len(shape))])
    return gain


def normal_values(stream_key, extent, scale, most, shards=(), kind=jnp.bfloat16):
    level = shard_levels(stream_key, extent, shards, -0.22, 0.18) if shards else 1.0
    drawn = jax.random.normal(stream_key, extent, jnp.float32) * scale * level
    return jnp.minimum(jnp.maximum(drawn, -most), most).astype(kind)


def setup_inputs(seed: int = 0) -> dict:
    streams_of = jax.random.split(jax.random.key(seed), 10)
    sky_image = normal_values(streams_of[0], (ROWS, CS), 1.0, 6.0, ((0, 16),))
    facet_rows = place_ends(jax.random.randint(streams_of[1], (N_FACET,), 0, NIMG - FS + 1), jax.random.fold_in(streams_of[1], 1), 0, NIMG - FS).astype(jnp.int32)
    column_offset = jax.random.randint(streams_of[2], (1,), 0, NIMG - M + 1).astype(jnp.int32)
    subgrid_offsets = jax.random.randint(streams_of[3], (SUBS,), 0, NIMG - M + 1).astype(jnp.int32)
    vis_u = place_ends(jax.random.randint(streams_of[4], (SUBS, VIS), 0, SUBW), jax.random.fold_in(streams_of[4], 1), 0, SUBW - 1).astype(jnp.int32)
    vis_v = place_ends(jax.random.randint(streams_of[5], (SUBS, VIS), 0, SUBW), jax.random.fold_in(streams_of[5], 1), 0, SUBW - 1).astype(jnp.int32)
    observed = normal_values(streams_of[6], (SUBS, 2, VIS), 1.0, 6.0, ((0, 2), (2, 16)), jnp.float32)
    weights = jnp.clip(jnp.exp(math.log(3.0) - 2.3025851 * jax.random.uniform(streams_of[7], (SUBS, VIS), jnp.float32) ** shard_levels(streams_of[7], (SUBS, VIS), ((0, 2), (1, 16)), -0.2, 0.2)), 0.3, 3.0)
    block_counts = place_ends(jax.random.randint(streams_of[8], (SUBS, N_FACET * N_BASE), 1, VB_DEV + 1), jax.random.fold_in(streams_of[8], 1), 1, VB_DEV).astype(jnp.int32)
    return {"sky_image": sky_image, "facet_rows": facet_rows, "column_offset": column_offset, "subgrid_offsets": subgrid_offsets, "vis_u": vis_u, "vis_v": vis_v, "observed": observed, "weights": weights, "block_counts": block_counts}


TWO_PI = 2.0 * math.pi


def modular_product(first_factor, second_factor):
    upper_part = second_factor // 256
    lower_part = second_factor % 256
    partial_mod = (first_factor * upper_part) % NIMG
    return ((partial_mod * 256) % NIMG + first_factor * lower_part) % NIMG


def phase_angle(first_factor, second_factor):
    return modular_product(first_factor, second_factor).astype(jnp.float32) * (TWO_PI / NIMG)


def grid_phase(first_factor, second_factor):
    return ((first_factor * second_factor) % SUBW).astype(jnp.float32) * (TWO_PI / SUBW)


def reference(sky_image, facet_rows, column_offset, subgrid_offsets, vis_u, vis_v, observed, weights, block_counts):
    row_ids = jnp.arange(ROWS, dtype=jnp.int32)
    row_pos = facet_rows[row_ids // FS] + row_ids % FS
    col_freq = column_offset[0] + jnp.arange(M, dtype=jnp.int32)
    col_angles = phase_angle(jnp.arange(CS, dtype=jnp.int32)[:, None], col_freq[None, :])
    col_table = (jnp.concatenate([jnp.cos(col_angles), -jnp.sin(col_angles)], axis=1) * (CS ** -0.5)).astype(jnp.bfloat16)
    spectrum = jnp.dot(sky_image, col_table, preferred_element_type=jnp.float32).astype(jnp.bfloat16)
    spectrum_rot = jnp.concatenate([spectrum[:, M:], -spectrum[:, :M]], axis=1)

    def predict(offset_row):
        frequencies = offset_row + jnp.arange(M, dtype=jnp.int32)
        angles = phase_angle(frequencies[:, None], row_pos[None, :])
        cosine = jnp.cos(angles).astype(jnp.bfloat16)
        sine_part = jnp.sin(angles).astype(jnp.bfloat16)
        summed = jnp.dot(cosine, spectrum, preferred_element_type=jnp.float32)
        summed = summed + jnp.dot(sine_part, spectrum_rot, preferred_element_type=jnp.float32)
        return (summed * (ROWS ** -0.5)).astype(jnp.bfloat16)

    subgrids = lax.map(predict, subgrid_offsets)

    shard_slots = VB_DEV * BLOCK
    slot_ids = jnp.arange(VIS, dtype=jnp.int32)
    shard_ids = slot_ids // shard_slots
    block_ids = (slot_ids % shard_slots) // BLOCK
    live_mask = block_ids[None, :] < block_counts[:, shard_ids]
    freq_ids = jnp.arange(M, dtype=jnp.int32)

    def visit_subgrid(inputs):
        grid_whole, along_u, along_v, seen_vis, weight_row, live_row = inputs
        angle_u = grid_phase(freq_ids[:, None], along_u[None, :])
        cos_along = jnp.cos(angle_u).astype(jnp.bfloat16)
        sin_along = jnp.sin(angle_u).astype(jnp.bfloat16)
        lookup = jnp.concatenate([jnp.concatenate([cos_along, -sin_along], axis=1),
                                  jnp.concatenate([sin_along, cos_along], axis=1)], axis=0)
        half_sums = jnp.dot(grid_whole, lookup, preferred_element_type=jnp.float32)
        angle_v = grid_phase(freq_ids[:, None], along_v[None, :])
        cos_rows = jnp.cos(angle_v).astype(jnp.bfloat16)
        sin_rows = jnp.sin(angle_v).astype(jnp.bfloat16)
        cos_wide = cos_rows.astype(jnp.float32)
        sin_wide = sin_rows.astype(jnp.float32)
        half_re = half_sums[:, :VIS]
        half_im = half_sums[:, VIS:]
        model_re = jnp.sum(cos_wide * half_re + sin_wide * half_im, axis=0)
        model_im = jnp.sum(cos_wide * half_im - sin_wide * half_re, axis=0)
        model_vis = jnp.stack([model_re, model_im]) * (1.0 / M)
        resid_vis = jnp.where(live_row[None, :], weight_row[None, :] * (seen_vis - model_vis), jnp.float32(0.0))
        rounded = resid_vis.astype(jnp.bfloat16).astype(jnp.float32)
        cos_cols = cos_along.astype(jnp.float32).T
        sin_cols = sin_along.astype(jnp.float32).T
        spread_re = cos_cols * rounded[0][:, None] - sin_cols * rounded[1][:, None]
        spread_im = sin_cols * rounded[0][:, None] + cos_cols * rounded[1][:, None]
        spread = jnp.concatenate([spread_re, spread_im], axis=1).astype(jnp.bfloat16)
        spread_rot = jnp.concatenate([-spread[:, M:], spread[:, :M]], axis=1)
        regrid = jnp.dot(cos_rows, spread, preferred_element_type=jnp.float32)
        regrid = regrid + jnp.dot(sin_rows, spread_rot, preferred_element_type=jnp.float32)
        return resid_vis, (regrid * (VIS ** -0.5)).astype(jnp.bfloat16)

    residual, regridded = lax.map(visit_subgrid, (subgrids, vis_u, vis_v, observed, weights, live_mask))

    def accumulate(running, inputs):
        offset_row, grid_whole = inputs
        frequencies = offset_row + jnp.arange(M, dtype=jnp.int32)
        angles = phase_angle(row_pos[:, None], frequencies[None, :])
        cosine = jnp.cos(angles).astype(jnp.bfloat16)
        sine_part = jnp.sin(angles).astype(jnp.bfloat16)
        grid_rot = jnp.concatenate([-grid_whole[:, M:], grid_whole[:, :M]], axis=1)
        running = running + jnp.dot(cosine, grid_whole, preferred_element_type=jnp.float32)
        running = running + jnp.dot(sine_part, grid_rot, preferred_element_type=jnp.float32)
        return running, None

    spectra, unused_out = lax.scan(accumulate, jnp.zeros((ROWS, 2 * M), jnp.float32), (subgrid_offsets, regridded))
    spectra = (spectra * ((SUBS * M) ** -0.5)).astype(jnp.bfloat16)
    out_angles = phase_angle(col_freq[:, None], jnp.arange(CS, dtype=jnp.int32)[None, :])
    out_table = (jnp.concatenate([jnp.cos(out_angles), -jnp.sin(out_angles)], axis=0) * (M ** -0.5)).astype(jnp.bfloat16)
    facet_update = jnp.dot(spectra, out_table, preferred_element_type=jnp.float32).astype(jnp.bfloat16)
    return residual, facet_update
```

```python
import functools
import math

import jax
import jax.numpy as jnp
from jax import lax
from jax.experimental import pallas as pl
from jax.experimental.pallas import tpu as pltpu
from jax.sharding import PartitionSpec as P

NIMG = 131072
M = 256
SUBW = 1024
BLOCK = 128
MESH = pl.DeviceIdType.MESH
F32 = jnp.float32
BF16 = jnp.bfloat16


def unit(first, second, period):
    half = period // 2
    turn = ((first * second + half) & (period - 1)) - half
    y = turn.astype(F32) * (math.pi / period)
    q = y * y
    s = F32(-1.0 / 39916800.0)
    for k in (362880.0, -5040.0, 120.0, -6.0):
        s = s * q + F32(1.0 / k)
    s = (s * q + F32(1.0)) * y
    c = F32(1.0 / 479001600.0)
    for k in (-3628800.0, 40320.0, -720.0, 24.0, -2.0):
        c = c * q + F32(1.0 / k)
    c = c * q + F32(1.0)
    return F32(1.0) - F32(2.0) * s * s, F32(2.0) * s * c


def rows_iota(count, step=1):
    return lax.broadcasted_iota(jnp.int32, (count, 1), 0) * step


def lanes_iota(count):
    return lax.broadcasted_iota(jnp.int32, (1, count), 1)


def phase_product(coarse, fine, put):
    coarse_cos, coarse_sin = coarse
    fine_cos, fine_sin = fine
    for a in range(coarse_cos.shape[0]):
        ca, sa = coarse_cos[a : a + 1, :], coarse_sin[a : a + 1, :]
        put(a, ca * fine_cos - sa * fine_sin, sa * fine_cos + ca * fine_sin)


def pieces(groups, cols):
    row_blocks = min(groups, M // 16)
    col_blocks = groups // row_blocks
    height, width = M // row_blocks, cols // col_blocks
    return [
        (r * col_blocks + c, r * height, c * width, height, width)
        for r in range(row_blocks)
        for c in range(col_blocks)
    ]


def halves(groups):
    return 2 if groups <= M // 16 else 1


def far_first(count):
    return sorted(range(1, count), key=lambda j: (-min(j, count - j), j))


def kernel(
    sizes,
    facet_rows,
    column_offset,
    subgrid_offsets,
    counts,
    sky_hbm,
    vis_u_hbm,
    vis_v_hbm,
    observed_hbm,
    weights_hbm,
    residual_out,
    update,
    sky,
    vis_u,
    vis_v,
    observed,
    weights,
    t1,
    spec,
    t2,
    du,
    dv,
    t5,
    t6,
    lhs,
    acc,
    spread,
    zed,
    partial,
    share,
    s_a,
    x_a,
    r_a,
    r_b,
    s_c,
    x_c,
    r_c,
    r_d,
    sky_sem,
    side_sem,
    send_sem,
    recv_sem,
    d_send,
    d_recv,
):
    n_facet, n_sub, n_base = sizes
    groups = n_facet * n_base
    parts = halves(groups)
    wide = 2 * M // parts
    half = wide // 2
    rows, columns = sky.shape
    tile = min(256, rows)
    vis = vis_u.shape[1]
    local_cols = update.shape[1]
    facet, sub, base = lax.axis_index("facet"), lax.axis_index("sub"), lax.axis_index("base")
    pairs = n_base // 2
    half_group = groups // 2
    plane = n_sub * pairs
    parity = lax.rem(base, 2)
    row_of_base = base // 2
    pair = facet * pairs + row_of_base
    spot = sub * pairs + row_of_base
    sibling = {"facet": facet, "sub": sub, "base": base + 1 - 2 * parity}

    def slot_of(g):
        f, b = g // n_base, g % n_base
        return (b % 2) * half_group + f * pairs + b // 2

    def d_slot(which, f, place):
        return (which * n_facet + f) * plane + place

    def mate(j):
        other = lax.rem(pair + j, half_group)
        return other, {
            "facet": other // pairs,
            "sub": sub,
            "base": lax.rem(other, pairs) * 2 + parity,
        }

    def level(j):
        other = lax.rem(spot + j, plane)
        return {"facet": facet, "sub": other // pairs, "base": lax.rem(other, pairs) * 2 + parity}

    def above(j):
        return {"facet": lax.rem(facet + j, n_facet), "sub": sub, "base": base}

    def each(indices, body):
        if len(indices) <= 16:
            for j in indices:
                body(j)
        else:
            pl.loop(min(indices), max(indices) + 1)(body)

    fetches = []
    for i in range(rows // tile):
        here = pl.ds(i * tile, tile)
        fetches.append(
            pltpu.make_async_copy(sky_hbm.at[here, :], sky.at[here, :], sky_sem.at[i])
        )
        fetches[i].start()
    sides = [
        pltpu.make_async_copy(source, target, side_sem.at[i])
        for i, (source, target) in enumerate(
            (
                (vis_u_hbm, vis_u),
                (vis_v_hbm, vis_v),
                (observed_hbm, observed),
                (weights_hbm, weights),
            )
        )
    ]
    for side in sides:
        side.start()
    barrier = pltpu.get_barrier_semaphore()

    def greet(device):
        pl.semaphore_signal(barrier, inc=1, device_id=device, device_id_type=MESH)

    greet(sibling)
    each(range(1, half_group), lambda j: greet(mate(j)[1]))

    def greet_level(j):
        other = lax.rem(sub + 1 + j // pairs, n_sub)
        greet({"facet": facet, "sub": other, "base": lax.rem(j, pairs) * 2 + parity})

    each(range((n_sub - 1) * pairs), greet_level)
    partners = 1 + (half_group - 1) + (n_sub - 1) * pairs

    def wait_all(phase, c, buffer, count):
        whole = buffer.at[c, pl.ds(0, count)]
        done = pltpu.make_async_remote_copy(
            whole, whole, send_sem.at[phase, c], recv_sem.at[phase, c], sibling, MESH
        )
        done.wait_recv()
        done.wait_send()

    def swap(phase, c, source, extra):
        theirs = source.at[c, pl.ds((1 - parity) * half_group, half_group)]
        return pltpu.make_async_remote_copy(
            theirs,
            extra.at[c],
            send_sem.at[phase, c],
            recv_sem.at[phase, c],
            sibling,
            MESH,
        )

    def scatter(phase, c, source, extra, landing):
        for i in range(half_group):
            at = parity * half_group + i
            joint = source[c, at].astype(F32) + extra[c, i].astype(F32)
            source[c, at] = joint.astype(BF16)

        def send(j):
            other, device = mate(j)
            pltpu.make_async_remote_copy(
                source.at[c, parity * half_group + other],
                landing.at[c, pair],
                send_sem.at[phase, c],
                recv_sem.at[phase, c],
                device,
                MESH,
            ).start()

        each(far_first(half_group), send)
        landing[c, pair] = source[c, parity * half_group + pair]

    def summed(landing, c):
        result = landing[c, 0].astype(F32)
        for g in range(1, half_group):
            result = result + landing[c, g].astype(F32)
        return result.astype(BF16)

    def gather(phase, c, buffer):
        slot = parity * half_group + pair

        def send(j):
            pltpu.make_async_remote_copy(
                buffer.at[c, slot],
                buffer.at[c, slot],
                send_sem.at[phase, c],
                recv_sem.at[phase, c],
                mate(j)[1],
                MESH,
            ).start()

        each(far_first(half_group), send)

    def relay(phase, c, buffer):
        mine = buffer.at[c, pl.ds(parity * half_group, half_group)]
        return pltpu.make_async_remote_copy(
            mine, mine, send_sem.at[phase, c], recv_sem.at[phase, c], sibling, MESH
        )

    def split(c, target, scale):
        for g, r, k, height, width in pieces(groups, wide):
            target[c, slot_of(g)] = (acc[r : r + height, k : k + width] * scale).astype(BF16)

    high = 128
    step = 32
    freq = column_offset[0] + lanes_iota(M)
    coarse_1 = unit(rows_iota(columns // high, high), freq, NIMG)
    fine_1 = unit(rows_iota(high), freq, NIMG)
    norm = F32(columns ** (-0.5))

    def make_t1(c):
        lanes = slice(c * half, (c + 1) * half)

        def put(a, cosine, sine):
            t1[c, a * high : (a + 1) * high, :half] = (cosine * norm).astype(BF16)
            t1[c, a * high : (a + 1) * high, half:] = (sine * -norm).astype(BF16)

        phase_product([x[:, lanes] for x in coarse_1], [x[:, lanes] for x in fine_1], put)

    row_start = facet_rows[facet] + base * rows

    def make_spec(c):
        for i in range(rows // tile):
            here = slice(i * tile, (i + 1) * tile)
            there = slice(rows + i * tile, rows + (i + 1) * tile)
            if not c and not i % 2:
                for later in fetches[i : i + 2]:
                    later.wait()
            part = jnp.dot(sky[here, :], t1[c], preferred_element_type=F32)
            real, imag = part[:, :half].astype(BF16), part[:, half:].astype(BF16)
            spec[c, here, :half] = real
            spec[c, here, half:] = imag
            spec[c, there, :half] = imag
            spec[c, there, half:] = -real

    def contribution(c):
        for i in range(2):
            here = slice(i * M // 2, (i + 1) * M // 2)
            acc[here, :] = jnp.dot(t2[here, :], spec[c], preferred_element_type=F32)
        split(c, s_a, F32((rows * groups) ** (-0.5)))

    fan = 16

    def grid_table(position, table):
        width = 512
        for at in range(0, vis, width):
            lanes = slice(at, at + width)
            place = position[0:1, lanes]
            coarse = unit(rows_iota(M // fan, fan), place, SUBW)
            fine = unit(rows_iota(fan), place, SUBW)

            def put(a, c, s):
                table[a * fan : (a + 1) * fan, lanes] = c.astype(BF16)
                table[M + a * fan : M + (a + 1) * fan, lanes] = s.astype(BF16)

            phase_product(coarse, fine, put)

    make_t1(0)
    positions = row_start + lanes_iota(rows)
    own_offset = subgrid_offsets[sub]
    coarse_2 = unit(own_offset + rows_iota(M // step, step), positions, NIMG)
    fine_2 = unit(rows_iota(step), positions, NIMG)

    def put_t2(a, c, s):
        t2[a * step : (a + 1) * step, :rows] = c.astype(BF16)
        t2[a * step : (a + 1) * step, rows:] = s.astype(BF16)

    phase_product(coarse_2, fine_2, put_t2)
    swaps = []
    for c in range(parts):
        make_spec(c)
        if c:
            swaps[c - 1].wait()
            scatter(1, c - 1, s_a, x_a, r_a)
        contribution(c)
        if not c:
            pl.semaphore_wait(barrier, partners)
        swaps.append(swap(0, c, s_a, x_a))
        swaps[c].start()
        if c + 1 < parts:
            make_t1(c + 1)
    for side in sides:
        side.wait()
    grid_table(vis_u, du)
    swaps[-1].wait()
    scatter(1, parts - 1, s_a, x_a, r_a)
    grid_table(vis_v, dv)
    for c in range(parts):
        wait_all(1, c, r_a, half_group - 1)
        r_b[c, parity * half_group + pair] = summed(r_a, c)
        gather(2, c, r_b)

    for s in range(n_sub):
        freqs = subgrid_offsets[s] + lanes_iota(M)
        coarse = unit(row_start + rows_iota(rows // high, high), freqs, NIMG)
        fine = unit(rows_iota(high), freqs, NIMG)

        def put_t5(a, c, sine, at=2 * M * s):
            t5[a * high : (a + 1) * high, at : at + M] = c.astype(BF16)
            t5[a * high : (a + 1) * high, at + M : at + 2 * M] = sine.astype(BF16)

        phase_product(coarse, fine, put_t5)

    relays = []
    for c in range(parts):
        wait_all(2, c, r_b, half_group - 1)
        relays.append(relay(3, c, r_b))
        relays[c].start()

    for c in range(parts):
        relays[c].wait()
        for g, r, k, height, width in pieces(groups, wide):
            block = r_b[c, slot_of(g)]
            part = min(width, half)
            for inner in range(0, width, part):
                value = block[:, inner : inner + part]
                at = k + inner
                if at < half:
                    re = c * half + at
                    lhs[r : r + height, re : re + part] = value
                    lhs[M + r : M + r + height, M + re : M + re + part] = -value
                else:
                    im = c * half + at - half
                    lhs[r : r + height, M + im : M + im + part] = value
                    lhs[M + r : M + r + height, im : im + part] = value

    chunk = 512
    live = counts[0, 0] * BLOCK

    for i in range(vis // chunk):
        lanes = slice(i * chunk, (i + 1) * chunk)
        both = jnp.dot(lhs[...], du[:, lanes], preferred_element_type=F32)
        both_re, both_im = both[:M], both[M:]
        cos_v, sin_v = dv[:M, lanes].astype(F32), dv[M:, lanes].astype(F32)
        model_re = jnp.sum(cos_v * both_re + sin_v * both_im, axis=0, keepdims=True)
        model_im = jnp.sum(cos_v * both_im - sin_v * both_re, axis=0, keepdims=True)
        alive = lanes_iota(chunk) + i * chunk < live
        weight = weights[0:1, lanes]
        inv = F32(1.0 / M)
        res_re = jnp.where(alive, weight * (observed[0, 0:1, lanes] - model_re * inv), F32(0.0))
        res_im = jnp.where(alive, weight * (observed[0, 1:2, lanes] - model_im * inv), F32(0.0))
        residual_out[0, 0:1, lanes] = res_re
        residual_out[0, 1:2, lanes] = res_im

    across = (((1,), (1,)), ((), ()))
    swaps = []
    for c in range(parts):
        for i in range(vis // chunk):
            lanes = slice(i * chunk, (i + 1) * chunk)
            r0 = residual_out[0, 0:1, lanes].astype(BF16).astype(F32)
            r1 = residual_out[0, 1:2, lanes].astype(BF16).astype(F32)
            cos_u = du[c * half : (c + 1) * half, lanes].astype(F32)
            sin_u = du[M + c * half : M + (c + 1) * half, lanes].astype(F32)
            spread[c, :half, lanes] = (cos_u * r0 - sin_u * r1).astype(BF16)
            spread[c, half:, lanes] = (sin_u * r0 + cos_u * r1).astype(BF16)
        for i in range(2):
            here = slice(i * M, (i + 1) * M)
            acc[here, :] = lax.dot_general(
                dv[here, :], spread[c], across, preferred_element_type=F32
            )
        acc[:M, :half] = acc[:M, :half] - acc[M:, half:]
        acc[:M, half:] = acc[:M, half:] + acc[M:, :half]
        if c:
            swaps[c - 1].wait()
            scatter(5, c - 1, s_c, x_c, r_c)
        split(c, s_c, F32((vis * groups) ** (-0.5)))
        swaps.append(swap(4, c, s_c, x_c))
        swaps[c].start()

    out_cols = sub * local_cols + lanes_iota(local_cols)
    coarse = unit(column_offset[0] + rows_iota(M // step, step), out_cols, NIMG)
    fine = unit(rows_iota(step), out_cols, NIMG)
    out_norm = F32(M ** (-0.5))

    def put_t6(a, c, s):
        which, at = a * step // half, a * step % half
        t6[which, at : at + step, :] = (c * out_norm).astype(BF16)
        t6[which, half + at : half + at + step, :] = (s * -out_norm).astype(BF16)

    phase_product(coarse, fine, put_t6)
    swaps[-1].wait()
    scatter(5, parts - 1, s_c, x_c, r_c)

    def column_copy(c, j, slot, device):
        piece = r_d.at[c, slot]
        return pltpu.make_async_remote_copy(
            piece, piece, d_send.at[0, c, j], d_recv.at[0, c, j], device, MESH
        )

    def level_sends(c, j):
        slot = d_slot(parity, lax.rem(facet + n_facet - j, n_facet), spot)

        def send(q):
            pltpu.make_async_remote_copy(
                r_d.at[c, slot],
                r_d.at[c, slot],
                d_send.at[1, c, j],
                d_recv.at[1, c, j],
                level(q),
                MESH,
            ).start()

        each(far_first(plane), send)

    def level_done(c, j):
        slot = d_slot(parity, lax.rem(facet + n_facet - j, n_facet), 0)
        several = r_d.at[c, pl.ds(slot, plane - 1)]
        return pltpu.make_async_remote_copy(
            several, several, d_send.at[1, c, j], d_recv.at[1, c, j], sibling, MESH
        )

    def level_relay(c, j):
        slot = d_slot(parity, lax.rem(facet + n_facet - j, n_facet), 0)
        slab = r_d.at[c, pl.ds(slot, plane)]
        return pltpu.make_async_remote_copy(
            slab, slab, d_send.at[2, c, j], d_recv.at[2, c, j], sibling, MESH
        )

    nearest = far_first(n_facet)[::-1]
    own = d_slot(parity, facet, spot)
    for c in range(parts):
        wait_all(5, c, r_c, half_group - 1)
        r_d[c, own] = summed(r_c, c)
        for j in nearest[::-1]:
            column_copy(c, j, own, above(j)).start()
        level_sends(c, 0)
    for c in range(parts):
        for j in nearest:
            slot = d_slot(parity, lax.rem(facet + n_facet - j, n_facet), spot)
            column_copy(c, j, slot, above(j)).wait_recv()
            level_sends(c, j)
    for c in range(parts):
        for j in [0] + nearest:
            level_done(c, j).wait_recv()
            level_relay(c, j).start()

    scale = F32((n_sub * M) ** (-0.5))
    for c in range(parts):
        for j in [0] + nearest:
            level_relay(c, j).wait_recv()
        for s in range(n_sub):
            top = 2 * M * s
            for g, r, k, height, width in pieces(groups, wide):
                f, b = g // n_base, g % n_base
                block = r_d[c, d_slot(b % 2, f, s * pairs + b // 2)]
                part = min(width, half)
                low = top + M + r
                for inner in range(0, width, part):
                    value = block[:, inner : inner + part]
                    at = k + inner
                    zed[c, top + r : top + r + height, at : at + part] = value
                    if at < half:
                        zed[c, low : low + height, half + at : half + at + part] = value
                    else:
                        zed[c, low : low + height, at - half : at - half + part] = -value
        for i in range(rows // tile):
            here = slice(i * tile, (i + 1) * tile)
            wave = jnp.dot(t5[here, :], zed[c], preferred_element_type=F32)
            share[here, :] = (wave * scale).astype(BF16)
        for i in range(rows // tile):
            here = slice(i * tile, (i + 1) * tile)
            term = jnp.dot(share[here, :], t6[c], preferred_element_type=F32)
            if c:
                term = partial[here, :] + term
            if c + 1 < parts:
                partial[here, :] = term
            else:
                update[here, :] = term.astype(BF16)

    for c in range(parts):
        for j in [0] + nearest:
            level_done(c, j).wait_send()
            level_relay(c, j).wait_send()
            if j:
                column_copy(c, j, own, above(j)).wait_send()


def shards(
    sizes,
    sky_image,
    facet_rows,
    column_offset,
    subgrid_offsets,
    vis_u,
    vis_v,
    observed,
    weights,
    block_counts,
):
    n_facet, n_sub, n_base = sizes
    groups = n_facet * n_base
    parts = halves(groups)
    wide = 2 * M // parts
    rows, columns = sky_image.shape
    vis = vis_u.shape[1]
    local_cols = columns // n_sub
    _, _, _, height, width = pieces(groups, wide)[0]
    smem = pl.BlockSpec(memory_space=pltpu.SMEM)
    vmem = pl.BlockSpec(memory_space=pltpu.VMEM)
    hbm = pl.BlockSpec(memory_space=pltpu.HBM)
    block = (parts, groups, height, width)
    half_block = (parts, groups // 2, height, width)
    return pl.pallas_call(
        functools.partial(kernel, sizes),
        out_shape=(
            pltpu.VMEM(observed.shape, F32),
            pltpu.VMEM((rows, local_cols), BF16),
        ),
        in_specs=[smem] * 4 + [hbm] * 5,
        out_specs=(vmem, vmem),
        scratch_shapes=[
            pltpu.VMEM((rows, columns), BF16),
            pltpu.VMEM(vis_u.shape, jnp.int32),
            pltpu.VMEM(vis_v.shape, jnp.int32),
            pltpu.VMEM(observed.shape, F32),
            pltpu.VMEM(weights.shape, F32),
            pltpu.VMEM((parts, columns, wide), BF16),
            pltpu.VMEM((parts, 2 * rows, wide), BF16),
            pltpu.VMEM((M, 2 * rows), BF16),
            pltpu.VMEM((2 * M, vis), BF16),
            pltpu.VMEM((2 * M, vis), BF16),
            pltpu.VMEM((rows, 2 * M * n_sub), BF16),
            pltpu.VMEM((parts, wide, local_cols), BF16),
            pltpu.VMEM((2 * M, 2 * M), BF16),
            pltpu.VMEM((2 * M, wide), F32),
            pltpu.VMEM((parts, wide, vis), BF16),
            pltpu.VMEM((parts, 2 * M * n_sub, wide), BF16),
            pltpu.VMEM((rows, local_cols), F32),
            pltpu.VMEM((rows, wide), BF16),
            pltpu.VMEM(block, BF16),
            pltpu.VMEM(half_block, BF16),
            pltpu.VMEM(half_block, BF16),
            pltpu.VMEM(block, BF16),
            pltpu.VMEM(block, BF16),
            pltpu.VMEM(half_block, BF16),
            pltpu.VMEM(half_block, BF16),
            pltpu.VMEM((parts, n_sub * groups, height, width), BF16),
            pltpu.SemaphoreType.DMA((rows // min(256, rows),)),
            pltpu.SemaphoreType.DMA((4,)),
            pltpu.SemaphoreType.DMA((6, parts)),
            pltpu.SemaphoreType.DMA((6, parts)),
            pltpu.SemaphoreType.DMA((3, parts, n_facet)),
            pltpu.SemaphoreType.DMA((3, parts, n_facet)),
        ],
        compiler_params=pltpu.CompilerParams(
            collective_id=0, has_side_effects=True, vmem_limit_bytes=56 * 1024 * 1024
        ),
        name="column",
    )(
        facet_rows,
        column_offset,
        subgrid_offsets,
        block_counts,
        sky_image,
        vis_u,
        vis_v,
        observed,
        weights,
    )


def solution(mesh):
    sizes = (mesh.shape["facet"], mesh.shape["sub"], mesh.shape["base"])
    return jax.shard_map(
        functools.partial(shards, sizes),
        mesh=mesh,
        in_specs=(
            P(("facet", "base"), None),
            P(),
            P(),
            P(),
            P("sub", ("facet", "base")),
            P("sub", ("facet", "base")),
            P("sub", None, ("facet", "base")),
            P("sub", ("facet", "base")),
            P("sub", ("facet", "base")),
        ),
        out_specs=(P("sub", None, ("facet", "base")), P(("facet", "base"), "sub")),
        check_vma=False,
    )
```

```python
import functools
import math

import jax
import jax.numpy as jnp
from jax import lax
from jax.experimental import pallas as pl
from jax.experimental.pallas import tpu as pltpu
from jax.sharding import PartitionSpec as P

NIMG = 131072
M = 256
SUBW = 1024
BLOCK = 128
MESH = pl.DeviceIdType.MESH
F32 = jnp.float32
BF16 = jnp.bfloat16


def unit(first, second, period):
    half = period // 2
    turn = ((first * second + half) & (period - 1)) - half
    y = turn.astype(F32) * (math.pi / period)
    q = y * y
    s = F32(-1.0 / 39916800.0)
    for k in (362880.0, -5040.0, 120.0, -6.0):
        s = s * q + F32(1.0 / k)
    s = (s * q + F32(1.0)) * y
    c = F32(1.0 / 479001600.0)
    for k in (-3628800.0, 40320.0, -720.0, 24.0, -2.0):
        c = c * q + F32(1.0 / k)
    c = c * q + F32(1.0)
    return F32(1.0) - F32(2.0) * s * s, F32(2.0) * s * c


def rows_iota(count, step=1):
    return lax.broadcasted_iota(jnp.int32, (count, 1), 0) * step


def lanes_iota(count):
    return lax.broadcasted_iota(jnp.int32, (1, count), 1)


def phase_product(coarse, fine, put):
    coarse_cos, coarse_sin = coarse
    fine_cos, fine_sin = fine
    for a in range(coarse_cos.shape[0]):
        ca, sa = coarse_cos[a : a + 1, :], coarse_sin[a : a + 1, :]
        put(a, ca * fine_cos - sa * fine_sin, sa * fine_cos + ca * fine_sin)


def pieces(groups, cols):
    row_blocks = min(groups, M // 16)
    col_blocks = groups // row_blocks
    height, width = M // row_blocks, cols // col_blocks
    return [
        (r * col_blocks + c, r * height, c * width, height, width)
        for r in range(row_blocks)
        for c in range(col_blocks)
    ]


def halves(groups):
    return 2 if groups <= M // 16 else 1


def far_first(count):
    return sorted(range(1, count), key=lambda j: (-min(j, count - j), j))


def kernel(
    sizes,
    facet_rows,
    column_offset,
    subgrid_offsets,
    counts,
    sky_hbm,
    vis_u_hbm,
    vis_v_hbm,
    observed_hbm,
    weights_hbm,
    residual_out,
    update,
    sky,
    vis_u,
    vis_v,
    observed,
    weights,
    t1,
    spec,
    t2,
    du,
    dv,
    t5,
    t6,
    lhs,
    model,
    acc,
    spread,
    zed,
    partial,
    share,
    s_a,
    x_a,
    r_a,
    r_b,
    s_c,
    x_c,
    r_c,
    r_d,
    sky_sem,
    side_sem,
    send_sem,
    recv_sem,
    d_send,
    d_recv,
):
    n_facet, n_sub, n_base = sizes
    groups = n_facet * n_base
    parts = halves(groups)
    wide = 2 * M // parts
    half = wide // 2
    rows, columns = sky.shape
    tile = min(256, rows)
    vis = vis_u.shape[1]
    local_cols = update.shape[1]
    facet, sub, base = lax.axis_index("facet"), lax.axis_index("sub"), lax.axis_index("base")
    pairs = n_base // 2
    half_group = groups // 2
    plane = n_sub * pairs
    parity = lax.rem(base, 2)
    row_of_base = base // 2
    pair = facet * pairs + row_of_base
    spot = sub * pairs + row_of_base
    sibling = {"facet": facet, "sub": sub, "base": base + 1 - 2 * parity}

    def d_slot(which, f, place):
        return (which * n_facet + f) * plane + place

    def by_distance(k):
        edge = lax.min(facet, n_facet - 1 - facet)
        across = facet + (k + 1) // 2 * (1 - k % 2 * 2)
        beyond = jnp.where(2 * facet < n_facet, k, n_facet - 1 - k)
        return jnp.where(k <= 2 * edge, across, beyond)

    sources = [facet] + [by_distance(k) for k in range(1, n_facet)]
    mates = [
        (f * pairs + q, {"facet": f, "sub": sub, "base": q * 2 + parity})
        for f in sources[:0:-1]
        for q in [lax.rem(row_of_base + d, pairs) for d in range(pairs)]
    ] + [
        (facet * pairs + q, {"facet": facet, "sub": sub, "base": q * 2 + parity})
        for q in [lax.rem(row_of_base + d, pairs) for d in range(1, pairs)]
    ]
    levels = [
        {"facet": facet, "sub": other // pairs, "base": lax.rem(other, pairs) * 2 + parity}
        for other in [lax.rem(spot + j, plane) for j in far_first(plane)]
    ]

    fetches = []
    for i in range(rows // tile):
        here = pl.ds(i * tile, tile)
        fetches.append(
            pltpu.make_async_copy(sky_hbm.at[here, :], sky.at[here, :], sky_sem.at[i])
        )
        fetches[i].start()
    sides = [
        pltpu.make_async_copy(source, target, side_sem.at[i])
        for i, (source, target) in enumerate(
            (
                (vis_u_hbm, vis_u),
                (vis_v_hbm, vis_v),
                (observed_hbm, observed),
                (weights_hbm, weights),
            )
        )
    ]
    for side in sides:
        side.start()
    barrier = pltpu.get_barrier_semaphore()

    def greet(device):
        pl.semaphore_signal(barrier, inc=1, device_id=device, device_id_type=MESH)

    greet(sibling)
    for _, device in mates:
        greet(device)
    for j in range((n_sub - 1) * pairs):
        other = lax.rem(sub + 1 + j // pairs, n_sub)
        greet({"facet": facet, "sub": other, "base": j % pairs * 2 + parity})
    partners = 1 + (half_group - 1) + (n_sub - 1) * pairs

    def wait_all(phase, c, buffer, count):
        whole = buffer.at[c, pl.ds(0, count)]
        done = pltpu.make_async_remote_copy(
            whole, whole, send_sem.at[phase, c], recv_sem.at[phase, c], sibling, MESH
        )
        done.wait_recv()
        done.wait_send()

    def swap(phase, c, source, extra):
        theirs = source.at[c, pl.ds((1 - parity) * half_group, half_group)]
        return pltpu.make_async_remote_copy(
            theirs,
            extra.at[c],
            send_sem.at[phase, c],
            recv_sem.at[phase, c],
            sibling,
            MESH,
        )

    def scatter(phase, c, source, extra, landing):
        for i in range(half_group):
            at = parity * half_group + i
            joint = source[c, at].astype(F32) + extra[c, i].astype(F32)
            source[c, at] = joint.astype(BF16)

        for other, device in mates:
            pltpu.make_async_remote_copy(
                source.at[c, parity * half_group + other],
                landing.at[c, pair],
                send_sem.at[phase, c],
                recv_sem.at[phase, c],
                device,
                MESH,
            ).start()
        landing[c, pair] = source[c, parity * half_group + pair]

    def summed(landing, c):
        result = landing[c, 0].astype(F32)
        for g in range(1, half_group):
            result = result + landing[c, g].astype(F32)
        return result.astype(BF16)

    def gather(phase, c, buffer):
        slot = parity * half_group + pair

        for _, device in mates:
            pltpu.make_async_remote_copy(
                buffer.at[c, slot],
                buffer.at[c, slot],
                send_sem.at[phase, c],
                recv_sem.at[phase, c],
                device,
                MESH,
            ).start()

    def relay(phase, c, buffer):
        mine = buffer.at[c, pl.ds(parity * half_group, half_group)]
        return pltpu.make_async_remote_copy(
            mine, mine, send_sem.at[phase, c], recv_sem.at[phase, c], sibling, MESH
        )

    def split(c, target, scale):
        for g, r, k, height, width in pieces(groups, wide):
            target[c, g] = (acc[r : r + height, k : k + width] * scale).astype(BF16)

    high = 128
    step = 32
    freq = column_offset[0] + lanes_iota(M)
    coarse_1 = unit(rows_iota(columns // high, high), freq, NIMG)
    fine_1 = unit(rows_iota(high), freq, NIMG)
    norm = F32(columns ** (-0.5))

    def make_t1(c):
        lanes = slice(c * half, (c + 1) * half)

        def put(a, cosine, sine):
            t1[c, a * high : (a + 1) * high, :half] = (cosine * norm).astype(BF16)
            t1[c, a * high : (a + 1) * high, half:] = (sine * -norm).astype(BF16)

        phase_product([x[:, lanes] for x in coarse_1], [x[:, lanes] for x in fine_1], put)

    row_start = facet_rows[facet] + base * rows

    def make_spec(c):
        for i in range(rows // tile):
            here = slice(i * tile, (i + 1) * tile)
            there = slice(rows + i * tile, rows + (i + 1) * tile)
            if not c and not i % 2:
                for later in fetches[i : i + 2]:
                    later.wait()
            part = jnp.dot(sky[here, :], t1[c], preferred_element_type=F32)
            real, imag = part[:, :half].astype(BF16), part[:, half:].astype(BF16)
            spec[c, here, :half] = real
            spec[c, here, half:] = imag
            spec[c, there, :half] = imag
            spec[c, there, half:] = -real

    def contribution(c):
        for i in range(2):
            here = slice(i * M // 2, (i + 1) * M // 2)
            acc[here, :] = jnp.dot(t2[here, :], spec[c], preferred_element_type=F32)
        split(c, s_a, F32((rows * groups) ** (-0.5)))

    fan = 16

    def grid_table(position, table):
        width = 512
        for at in range(0, vis, width):
            lanes = slice(at, at + width)
            place = position[0:1, lanes]
            coarse = unit(rows_iota(M // fan, fan), place, SUBW)
            fine = unit(rows_iota(fan), place, SUBW)

            def put(a, c, s):
                table[a * fan : (a + 1) * fan, lanes] = c.astype(BF16)
                table[M + a * fan : M + (a + 1) * fan, lanes] = s.astype(BF16)

            phase_product(coarse, fine, put)

    make_t1(0)
    positions = row_start + lanes_iota(rows)
    own_offset = subgrid_offsets[sub]
    coarse_2 = unit(own_offset + rows_iota(M // step, step), positions, NIMG)
    fine_2 = unit(rows_iota(step), positions, NIMG)

    def put_t2(a, c, s):
        t2[a * step : (a + 1) * step, :rows] = c.astype(BF16)
        t2[a * step : (a + 1) * step, rows:] = s.astype(BF16)

    phase_product(coarse_2, fine_2, put_t2)
    swaps = []
    for c in range(parts):
        make_spec(c)
        if c:
            swaps[c - 1].wait()
            scatter(1, c - 1, s_a, x_a, r_a)
        contribution(c)
        if not c:
            pl.semaphore_wait(barrier, partners)
        swaps.append(swap(0, c, s_a, x_a))
        swaps[c].start()
        if c + 1 < parts:
            make_t1(c + 1)
    for side in sides:
        side.wait()
    grid_table(vis_u, du)
    swaps[-1].wait()
    scatter(1, parts - 1, s_a, x_a, r_a)
    grid_table(vis_v, dv)
    for c in range(parts):
        wait_all(1, c, r_a, half_group - 1)
        r_b[c, parity * half_group + pair] = summed(r_a, c)
        gather(2, c, r_b)

    for s in range(n_sub):
        freqs = subgrid_offsets[s] + lanes_iota(M)
        coarse = unit(row_start + rows_iota(rows // high, high), freqs, NIMG)
        fine = unit(rows_iota(high), freqs, NIMG)

        def put_t5(a, c, sine, at=2 * M * s):
            t5[a * high : (a + 1) * high, at : at + M] = c.astype(BF16)
            t5[a * high : (a + 1) * high, at + M : at + 2 * M] = sine.astype(BF16)

        phase_product(coarse, fine, put_t5)

    relays = []
    for c in range(parts):
        wait_all(2, c, r_b, half_group - 1)
        relays.append(relay(3, c, r_b))
        relays[c].start()

    top = M // 2

    def make_lhs(which, c):
        for g, r, k, height, width in pieces(groups, wide)[:half_group]:
            block = r_b[c, which * half_group + g]
            part = min(width, half)
            for inner in range(0, width, part):
                value = block[:, inner : inner + part]
                at = k + inner
                if at < half:
                    re = c * half + at
                    lhs[which, r : r + height, re : re + part] = value
                    lhs[which, top + r : top + r + height, M + re : M + re + part] = -value
                else:
                    im = c * half + at - half
                    lhs[which, r : r + height, M + im : M + im + part] = value
                    lhs[which, top + r : top + r + height, im : im + part] = value

    chunk = 512
    live = counts[0, 0] * BLOCK

    def model_terms(which, lanes):
        both = jnp.dot(lhs[which], du[:, lanes], preferred_element_type=F32)
        both_re, both_im = both[:top], both[top:]
        cos_v = dv[pl.ds(pl.multiple_of(which * top, top), top), lanes].astype(F32)
        sin_v = dv[pl.ds(pl.multiple_of(M + which * top, top), top), lanes].astype(F32)
        return (
            jnp.sum(cos_v * both_re + sin_v * both_im, axis=0, keepdims=True),
            jnp.sum(cos_v * both_im - sin_v * both_re, axis=0, keepdims=True),
        )

    for c in range(parts):
        make_lhs(parity, c)
    for i in range(vis // chunk):
        lanes = slice(i * chunk, (i + 1) * chunk)
        model[0:1, lanes], model[1:2, lanes] = model_terms(parity, lanes)
    for c in range(parts):
        relays[c].wait()
    for c in range(parts):
        make_lhs(1 - parity, c)
    for i in range(vis // chunk):
        lanes = slice(i * chunk, (i + 1) * chunk)
        model_re, model_im = model_terms(1 - parity, lanes)
        model_re, model_im = model_re + model[0:1, lanes], model_im + model[1:2, lanes]
        alive = lanes_iota(chunk) + i * chunk < live
        weight = weights[0:1, lanes]
        inv = F32(1.0 / M)
        res_re = jnp.where(alive, weight * (observed[0, 0:1, lanes] - model_re * inv), F32(0.0))
        res_im = jnp.where(alive, weight * (observed[0, 1:2, lanes] - model_im * inv), F32(0.0))
        residual_out[0, 0:1, lanes] = res_re
        residual_out[0, 1:2, lanes] = res_im

    across = (((1,), (1,)), ((), ()))
    swaps = []
    for c in range(parts):
        for i in range(vis // chunk):
            lanes = slice(i * chunk, (i + 1) * chunk)
            r0 = residual_out[0, 0:1, lanes].astype(BF16)
            r1 = residual_out[0, 1:2, lanes].astype(BF16)
            cos_u = du[c * half : (c + 1) * half, lanes]
            sin_u = du[M + c * half : M + (c + 1) * half, lanes]
            spread[c, :half, lanes] = cos_u * r0 - sin_u * r1
            spread[c, half:, lanes] = sin_u * r0 + cos_u * r1
        for i in range(2):
            here = slice(i * M, (i + 1) * M)
            acc[here, :] = lax.dot_general(
                dv[here, :], spread[c], across, preferred_element_type=F32
            )
        acc[:M, :half] = acc[:M, :half] - acc[M:, half:]
        acc[:M, half:] = acc[:M, half:] + acc[M:, :half]
        if c:
            swaps[c - 1].wait()
            scatter(5, c - 1, s_c, x_c, r_c)
        split(c, s_c, F32((vis * groups) ** (-0.5)))
        swaps.append(swap(4, c, s_c, x_c))
        swaps[c].start()

    out_cols = sub * local_cols + lanes_iota(local_cols)
    coarse = unit(column_offset[0] + rows_iota(M // step, step), out_cols, NIMG)
    fine = unit(rows_iota(step), out_cols, NIMG)
    out_norm = F32(M ** (-0.5))

    def put_t6(a, c, s):
        which, at = a * step // half, a * step % half
        t6[which, at : at + step, :] = (c * out_norm).astype(BF16)
        t6[which, half + at : half + at + step, :] = (s * -out_norm).astype(BF16)

    phase_product(coarse, fine, put_t6)
    swaps[-1].wait()
    scatter(5, parts - 1, s_c, x_c, r_c)

    def slab(c, f, count):
        return r_d.at[c, pl.ds(d_slot(parity, f, 0), count)]

    def column_copy(c, k, f, device, arrived):
        piece = r_d.at[c, d_slot(parity, f, spot)]
        return pltpu.make_async_remote_copy(
            piece, piece, d_send.at[0, c, k], d_recv.at[0, c, arrived], device, MESH
        )

    def level_copy(c, f, piece, device):
        return pltpu.make_async_remote_copy(
            piece, piece, d_send.at[1, c, f], d_recv.at[1, c, f], device, MESH
        )

    def level_sends(c, f):
        for device in levels:
            level_copy(c, f, r_d.at[c, d_slot(parity, f, spot)], device).start()

    def level_done(c, f):
        return level_copy(c, f, slab(c, f, plane - 1), sibling)

    def level_relay(c, f):
        whole = slab(c, f, plane)
        return pltpu.make_async_remote_copy(
            whole, whole, d_send.at[2, c, f], d_recv.at[2, c, f], sibling, MESH
        )

    for c in range(parts):
        wait_all(5, c, r_c, half_group - 1)
        r_d[c, d_slot(parity, facet, spot)] = summed(r_c, c)
        for k in range(n_facet - 1, 0, -1):
            device = {"facet": sources[k], "sub": sub, "base": base}
            column_copy(c, k, facet, device, facet).start()
        level_sends(c, facet)
    for c in range(parts):
        for k in range(1, n_facet):
            column_copy(c, k, sources[k], sibling, sources[k]).wait_recv()
            level_sends(c, sources[k])
    for c in range(parts):
        for f in sources:
            level_done(c, f).wait_recv()
            level_relay(c, f).start()

    scale = F32((n_sub * M) ** (-0.5))
    for c in range(parts):
        for f in sources:
            level_relay(c, f).wait_recv()
        for s in range(n_sub):
            top = 2 * M * s
            for g, r, k, height, width in pieces(groups, wide):
                which, place = g // half_group, g % half_group
                block = r_d[c, d_slot(which, place // pairs, s * pairs + place % pairs)]
                part = min(width, half)
                low = top + M + r
                for inner in range(0, width, part):
                    value = block[:, inner : inner + part]
                    at = k + inner
                    zed[c, top + r : top + r + height, at : at + part] = value
                    if at < half:
                        zed[c, low : low + height, half + at : half + at + part] = value
                    else:
                        zed[c, low : low + height, at - half : at - half + part] = -value
        for i in range(rows // tile):
            here = slice(i * tile, (i + 1) * tile)
            wave = jnp.dot(t5[here, :], zed[c], preferred_element_type=F32)
            share[here, :] = (wave * scale).astype(BF16)
        for i in range(rows // tile):
            here = slice(i * tile, (i + 1) * tile)
            term = jnp.dot(share[here, :], t6[c], preferred_element_type=F32)
            if c:
                term = partial[here, :] + term
            if c + 1 < parts:
                partial[here, :] = term
            else:
                update[here, :] = term.astype(BF16)

    for c in range(parts):
        for k in range(n_facet):
            level_done(c, sources[k]).wait_send()
            level_relay(c, sources[k]).wait_send()
            if k:
                column_copy(c, k, facet, sibling, facet).wait_send()


def deliver(residual, update, residual_out, update_out, sems):
    copies = [
        pltpu.make_async_copy(residual, residual_out, sems.at[0]),
        pltpu.make_async_copy(update, update_out, sems.at[1]),
    ]
    for copy in copies:
        copy.start()
    for copy in copies:
        copy.wait()


def shards(
    sizes,
    sky_image,
    facet_rows,
    column_offset,
    subgrid_offsets,
    vis_u,
    vis_v,
    observed,
    weights,
    block_counts,
):
    n_facet, n_sub, n_base = sizes
    groups = n_facet * n_base
    parts = halves(groups)
    wide = 2 * M // parts
    rows, columns = sky_image.shape
    vis = vis_u.shape[1]
    local_cols = columns // n_sub
    _, _, _, height, width = pieces(groups, wide)[0]
    smem = pl.BlockSpec(memory_space=pltpu.SMEM)
    vmem = pl.BlockSpec(memory_space=pltpu.VMEM)
    hbm = pl.BlockSpec(memory_space=pltpu.HBM)
    block = (parts, groups, height, width)
    half_block = (parts, groups // 2, height, width)
    residual, update = pl.pallas_call(
        functools.partial(kernel, sizes),
        out_shape=(
            pltpu.VMEM(observed.shape, F32),
            pltpu.VMEM((rows, local_cols), BF16),
        ),
        in_specs=[smem] * 4 + [hbm] * 5,
        out_specs=(vmem, vmem),
        scratch_shapes=[
            pltpu.VMEM((rows, columns), BF16),
            pltpu.VMEM(vis_u.shape, jnp.int32),
            pltpu.VMEM(vis_v.shape, jnp.int32),
            pltpu.VMEM(observed.shape, F32),
            pltpu.VMEM(weights.shape, F32),
            pltpu.VMEM((parts, columns, wide), BF16),
            pltpu.VMEM((parts, 2 * rows, wide), BF16),
            pltpu.VMEM((M, 2 * rows), BF16),
            pltpu.VMEM((2 * M, vis), BF16),
            pltpu.VMEM((2 * M, vis), BF16),
            pltpu.VMEM((rows, 2 * M * n_sub), BF16),
            pltpu.VMEM((parts, wide, local_cols), BF16),
            pltpu.VMEM((2, M, 2 * M), BF16),
            pltpu.VMEM((2, vis), F32),
            pltpu.VMEM((2 * M, wide), F32),
            pltpu.VMEM((parts, wide, vis), BF16),
            pltpu.VMEM((parts, 2 * M * n_sub, wide), BF16),
            pltpu.VMEM((rows, local_cols), F32),
            pltpu.VMEM((rows, wide), BF16),
            pltpu.VMEM(block, BF16),
            pltpu.VMEM(half_block, BF16),
            pltpu.VMEM(half_block, BF16),
            pltpu.VMEM(block, BF16),
            pltpu.VMEM(block, BF16),
            pltpu.VMEM(half_block, BF16),
            pltpu.VMEM(half_block, BF16),
            pltpu.VMEM((parts, n_sub * groups, height, width), BF16),
            pltpu.SemaphoreType.DMA((rows // min(256, rows),)),
            pltpu.SemaphoreType.DMA((4,)),
            pltpu.SemaphoreType.DMA((6, parts)),
            pltpu.SemaphoreType.DMA((6, parts)),
            pltpu.SemaphoreType.DMA((3, parts, n_facet)),
            pltpu.SemaphoreType.DMA((3, parts, n_facet)),
        ],
        compiler_params=pltpu.CompilerParams(
            collective_id=0, has_side_effects=True, vmem_limit_bytes=56 * 1024 * 1024
        ),
        name="column",
    )(
        facet_rows,
        column_offset,
        subgrid_offsets,
        block_counts,
        sky_image,
        vis_u,
        vis_v,
        observed,
        weights,
    )
    return pl.pallas_call(
        deliver,
        out_shape=(
            jax.ShapeDtypeStruct(residual.shape, F32),
            jax.ShapeDtypeStruct(update.shape, BF16),
        ),
        in_specs=[vmem] * 2,
        out_specs=(hbm, hbm),
        scratch_shapes=[pltpu.SemaphoreType.DMA((2,))],
        name="deliver",
    )(
        pltpu.with_memory_space_constraint(residual, pltpu.VMEM),
        pltpu.with_memory_space_constraint(update, pltpu.VMEM),
    )


def solution(mesh):
    sizes = (mesh.shape["facet"], mesh.shape["sub"], mesh.shape["base"])
    return jax.shard_map(
        functools.partial(shards, sizes),
        mesh=mesh,
        in_specs=(
            P(("facet", "base"), None),
            P(),
            P(),
            P(),
            P("sub", ("facet", "base")),
            P("sub", ("facet", "base")),
            P("sub", None, ("facet", "base")),
            P("sub", ("facet", "base")),
            P("sub", ("facet", "base")),
        ),
        out_specs=(P("sub", None, ("facet", "base")), P(("facet", "base"), "sub")),
        check_vma=False,
    )
```

```python
import functools
import math

import jax
import jax.numpy as jnp
from jax import lax
from jax.experimental import pallas as pl
from jax.experimental.pallas import tpu as pltpu
from jax.sharding import PartitionSpec as P

NIMG = 131072
M = 256
SUBW = 1024
BLOCK = 128
MESH = pl.DeviceIdType.MESH
F32 = jnp.float32
BF16 = jnp.bfloat16


def unit(first, second, period):
    half = period // 2
    turn = ((first * second + half) & (period - 1)) - half
    y = turn.astype(F32) * (math.pi / period)
    q = y * y
    s = F32(-1.0 / 39916800.0)
    for k in (362880.0, -5040.0, 120.0, -6.0):
        s = s * q + F32(1.0 / k)
    s = (s * q + F32(1.0)) * y
    c = F32(1.0 / 479001600.0)
    for k in (-3628800.0, 40320.0, -720.0, 24.0, -2.0):
        c = c * q + F32(1.0 / k)
    c = c * q + F32(1.0)
    return F32(1.0) - F32(2.0) * s * s, F32(2.0) * s * c


def rows_iota(count, step=1):
    return lax.broadcasted_iota(jnp.int32, (count, 1), 0) * step


def lanes_iota(count):
    return lax.broadcasted_iota(jnp.int32, (1, count), 1)


def phase_product(coarse, fine, put):
    coarse_cos, coarse_sin = coarse
    fine_cos, fine_sin = fine
    for a in range(coarse_cos.shape[0]):
        ca, sa = coarse_cos[a : a + 1, :], coarse_sin[a : a + 1, :]
        put(a, ca * fine_cos - sa * fine_sin, sa * fine_cos + ca * fine_sin)


def pieces(groups, cols):
    row_blocks = min(groups, M // 16)
    col_blocks = groups // row_blocks
    height, width = M // row_blocks, cols // col_blocks
    return [
        (r * col_blocks + c, r * height, c * width, height, width)
        for r in range(row_blocks)
        for c in range(col_blocks)
    ]


def halves(groups):
    return 2 if groups <= M // 16 else 1


def layers(n_facet, groups):
    return n_facet if groups <= M // 16 else 1


def far_first(count):
    return sorted(range(1, count), key=lambda j: (-min(j, count - j), j))


def kernel(
    sizes,
    facet_rows_hbm,
    column_offset,
    subgrid_offsets_hbm,
    counts,
    sky_hbm,
    vis_u_hbm,
    vis_v_hbm,
    observed_hbm,
    weights_hbm,
    residual_out,
    t5,
    t6,
    zed,
    partial,
    wave,
    facet_rows,
    subgrid_offsets,
    sky,
    vis_u,
    vis_v,
    observed,
    weights,
    t1,
    spec,
    t2,
    du,
    dv,
    lhs,
    model,
    acc,
    spread,
    share,
    s_a,
    x_a,
    r_a,
    r_b,
    s_c,
    x_c,
    r_c,
    r_d,
    sky_sem,
    side_sem,
    small_sem,
    send_sem,
    recv_sem,
    d_send,
    d_recv,
):
    n_facet, n_sub, n_base = sizes
    groups = n_facet * n_base
    parts = halves(groups)
    wide = 2 * M // parts
    half = wide // 2
    stages = layers(n_facet, groups)
    rows, columns = sky.shape
    tile = min(256, rows)
    vis = vis_u.shape[1]
    local_cols = t6.shape[2]
    facet, sub, base = lax.axis_index("facet"), lax.axis_index("sub"), lax.axis_index("base")
    pairs = n_base // 2
    half_group = groups // 2
    plane = n_sub * pairs
    parity = lax.rem(base, 2)
    row_of_base = base // 2
    pair = facet * pairs + row_of_base
    spot = sub * pairs + row_of_base
    sibling = {"facet": facet, "sub": sub, "base": base + 1 - 2 * parity}

    def d_slot(which, f, place):
        return (which * n_facet + f) * plane + place

    def by_distance(k):
        edge = lax.min(facet, n_facet - 1 - facet)
        across = facet + (k + 1) // 2 * (1 - k % 2 * 2)
        beyond = jnp.where(2 * facet < n_facet, k, n_facet - 1 - k)
        return jnp.where(k <= 2 * edge, across, beyond)

    sources = [facet] + [by_distance(k) for k in range(1, n_facet)]
    mates = [
        (f * pairs + q, {"facet": f, "sub": sub, "base": q * 2 + parity})
        for f in sources[:0:-1]
        for q in [lax.rem(row_of_base + d, pairs) for d in range(pairs)]
    ] + [
        (facet * pairs + q, {"facet": facet, "sub": sub, "base": q * 2 + parity})
        for q in [lax.rem(row_of_base + d, pairs) for d in range(1, pairs)]
    ]
    steps = [(a, b) for a in range(n_sub) for b in range(pairs)][1:]
    steps.sort(key=lambda ab: (not (ab[0] and ab[1]), bool(ab[0])))
    levels = [
        {
            "facet": facet,
            "sub": lax.rem(sub + a, n_sub),
            "base": lax.rem(row_of_base + b, pairs) * 2 + parity,
        }
        for a, b in steps
    ]

    smalls = [
        pltpu.make_async_copy(source, target, small_sem.at[i])
        for i, (source, target) in enumerate(
            (
                (facet_rows_hbm, facet_rows),
                (subgrid_offsets_hbm, subgrid_offsets),
            )
        )
    ]
    for small in smalls:
        small.start()
    fetches = []
    for i in range(rows // tile):
        here = pl.ds(i * tile, tile)
        fetches.append(
            pltpu.make_async_copy(sky_hbm.at[here, :], sky.at[here, :], sky_sem.at[i])
        )
        fetches[i].start()
    sides = [
        pltpu.make_async_copy(source, target, side_sem.at[i])
        for i, (source, target) in enumerate(
            (
                (vis_u_hbm, vis_u),
                (vis_v_hbm, vis_v),
                (observed_hbm, observed),
                (weights_hbm, weights),
            )
        )
    ]
    for side in sides:
        side.start()
    barrier = pltpu.get_barrier_semaphore()

    def greet(device):
        pl.semaphore_signal(barrier, inc=1, device_id=device, device_id_type=MESH)

    greet(sibling)
    for _, device in mates:
        greet(device)
    for j in range((n_sub - 1) * pairs):
        other = lax.rem(sub + 1 + j // pairs, n_sub)
        greet({"facet": facet, "sub": other, "base": j % pairs * 2 + parity})
    partners = 1 + (half_group - 1) + (n_sub - 1) * pairs

    def wait_all(phase, c, buffer, count):
        whole = buffer.at[c, pl.ds(0, count)]
        done = pltpu.make_async_remote_copy(
            whole, whole, send_sem.at[phase, c], recv_sem.at[phase, c], sibling, MESH
        )
        done.wait_recv()
        done.wait_send()

    def swap(phase, c, source, extra):
        theirs = source.at[c, pl.ds((1 - parity) * half_group, half_group)]
        return pltpu.make_async_remote_copy(
            theirs,
            extra.at[c],
            send_sem.at[phase, c],
            recv_sem.at[phase, c],
            sibling,
            MESH,
        )

    def scatter(phase, c, source, extra, landing):
        for i in range(half_group):
            at = parity * half_group + i
            joint = source[c, at].astype(F32) + extra[c, i].astype(F32)
            source[c, at] = joint.astype(BF16)

        for other, device in mates:
            pltpu.make_async_remote_copy(
                source.at[c, parity * half_group + other],
                landing.at[c, pair],
                send_sem.at[phase, c],
                recv_sem.at[phase, c],
                device,
                MESH,
            ).start()
        landing[c, pair] = source[c, parity * half_group + pair]

    def summed(landing, c):
        result = landing[c, 0].astype(F32)
        for g in range(1, half_group):
            result = result + landing[c, g].astype(F32)
        return result.astype(BF16)

    def gather(phase, c, buffer):
        slot = parity * half_group + pair

        for _, device in mates:
            pltpu.make_async_remote_copy(
                buffer.at[c, slot],
                buffer.at[c, slot],
                send_sem.at[phase, c],
                recv_sem.at[phase, c],
                device,
                MESH,
            ).start()

    def relay(phase, c, buffer):
        mine = buffer.at[c, pl.ds(parity * half_group, half_group)]
        return pltpu.make_async_remote_copy(
            mine, mine, send_sem.at[phase, c], recv_sem.at[phase, c], sibling, MESH
        )

    def split(c, target, scale):
        for g, r, k, height, width in pieces(groups, wide):
            target[c, g] = (acc[r : r + height, k : k + width] * scale).astype(BF16)

    high = 128
    step = 32
    freq = column_offset[0] + lanes_iota(M)
    coarse_1 = unit(rows_iota(columns // high, high), freq, NIMG)
    fine_1 = unit(rows_iota(high), freq, NIMG)
    norm = F32(columns ** (-0.5))

    def make_t1(c):
        lanes = slice(c * half, (c + 1) * half)

        def put(a, cosine, sine):
            t1[c, a * high : (a + 1) * high, :half] = (cosine * norm).astype(BF16)
            t1[c, a * high : (a + 1) * high, half:] = (sine * -norm).astype(BF16)

        phase_product([x[:, lanes] for x in coarse_1], [x[:, lanes] for x in fine_1], put)

    def make_spec(c):
        for i in range(rows // tile):
            here = slice(i * tile, (i + 1) * tile)
            there = slice(rows + i * tile, rows + (i + 1) * tile)
            if not c and not i % 2:
                for later in fetches[i : i + 2]:
                    later.wait()
            part = jnp.dot(sky[here, :], t1[c], preferred_element_type=F32)
            real, imag = part[:, :half].astype(BF16), part[:, half:].astype(BF16)
            spec[c, here, :half] = real
            spec[c, here, half:] = imag
            spec[c, there, :half] = imag
            spec[c, there, half:] = -real

    def contribution(c):
        for i in range(2):
            here = slice(i * M // 2, (i + 1) * M // 2)
            acc[here, :] = jnp.dot(t2[here, :], spec[c], preferred_element_type=F32)
        split(c, s_a, F32((rows * groups) ** (-0.5)))

    fan = 16

    def grid_table(position, table):
        width = 512
        for at in range(0, vis, width):
            lanes = slice(at, at + width)
            place = position[0:1, lanes]
            coarse = unit(rows_iota(M // fan, fan), place, SUBW)
            fine = unit(rows_iota(fan), place, SUBW)

            def put(a, c, s):
                table[a * fan : (a + 1) * fan, lanes] = c.astype(BF16)
                table[M + a * fan : M + (a + 1) * fan, lanes] = s.astype(BF16)

            phase_product(coarse, fine, put)

    for c in range(parts):
        make_t1(c)
    for small in smalls:
        small.wait()
    row_start = facet_rows[facet] + base * rows
    positions = row_start + lanes_iota(rows)
    own_offset = subgrid_offsets[sub]
    coarse_2 = unit(own_offset + rows_iota(M // step, step), positions, NIMG)
    fine_2 = unit(rows_iota(step), positions, NIMG)

    def put_t2(a, c, s):
        t2[a * step : (a + 1) * step, :rows] = c.astype(BF16)
        t2[a * step : (a + 1) * step, rows:] = s.astype(BF16)

    phase_product(coarse_2, fine_2, put_t2)

    swaps = []
    for c in range(parts):
        make_spec(c)
        contribution(c)
        if not c:
            pl.semaphore_wait(barrier, partners)
        swaps.append(swap(0, c, s_a, x_a))
        swaps[c].start()
        if c:
            swaps[c - 1].wait()
            scatter(1, c - 1, s_a, x_a, r_a)
    for side in sides:
        side.wait()
    grid_table(vis_u, du)
    swaps[-1].wait()
    scatter(1, parts - 1, s_a, x_a, r_a)
    grid_table(vis_v, dv)
    for c in range(parts):
        wait_all(1, c, r_a, half_group - 1)
        r_b[c, parity * half_group + pair] = summed(r_a, c)
        gather(2, c, r_b)

    span = M // 2 // stages
    run = n_sub * 2 * span
    lane = lanes_iota(run)
    start = lax.rem(lane // span, 2) * (M // 2) + lax.rem(lane, span)
    for s in range(n_sub):
        start = start + jnp.where(lane // (2 * span) == s, subgrid_offsets[s], 0)
    for k in range(stages):
        freqs = start + sources[k] * span if stages > 1 else start
        coarse = unit(row_start + rows_iota(rows // high, high), freqs, NIMG)
        fine = unit(rows_iota(high), freqs, NIMG)

        def put_t5(a, c, sine, at=2 * run * k):
            t5[a * high : (a + 1) * high, at : at + run] = c.astype(BF16)
            t5[a * high : (a + 1) * high, at + run : at + 2 * run] = sine.astype(BF16)

        phase_product(coarse, fine, put_t5)

    relays = []
    for c in range(parts):
        wait_all(2, c, r_b, half_group - 1)
        relays.append(relay(3, c, r_b))
        relays[c].start()

    top = M // 2

    def make_lhs(which, c):
        for g, r, k, height, width in pieces(groups, wide)[:half_group]:
            block = r_b[c, which * half_group + g]
            part = min(width, half)
            for inner in range(0, width, part):
                value = block[:, inner : inner + part]
                at = k + inner
                if at < half:
                    re = c * half + at
                    lhs[which, r : r + height, re : re + part] = value
                    lhs[which, top + r : top + r + height, M + re : M + re + part] = -value
                else:
                    im = c * half + at - half
                    lhs[which, r : r + height, M + im : M + im + part] = value
                    lhs[which, top + r : top + r + height, im : im + part] = value

    chunk = 512
    live = counts[0, 0] * BLOCK

    def model_terms(which, lanes):
        both = jnp.dot(lhs[which], du[:, lanes], preferred_element_type=F32)
        both_re, both_im = both[:top], both[top:]
        cos_v = dv[pl.ds(pl.multiple_of(which * top, top), top), lanes].astype(F32)
        sin_v = dv[pl.ds(pl.multiple_of(M + which * top, top), top), lanes].astype(F32)
        return (
            jnp.sum(cos_v * both_re + sin_v * both_im, axis=0, keepdims=True),
            jnp.sum(cos_v * both_im - sin_v * both_re, axis=0, keepdims=True),
        )

    for c in range(parts):
        make_lhs(parity, c)
    for i in range(vis // chunk):
        lanes = slice(i * chunk, (i + 1) * chunk)
        model[0:1, lanes], model[1:2, lanes] = model_terms(parity, lanes)
    for c in range(parts):
        relays[c].wait()
    for c in range(parts):
        make_lhs(1 - parity, c)
    for i in range(vis // chunk):
        lanes = slice(i * chunk, (i + 1) * chunk)
        model_re, model_im = model_terms(1 - parity, lanes)
        model_re, model_im = model_re + model[0:1, lanes], model_im + model[1:2, lanes]
        alive = lanes_iota(chunk) + i * chunk < live
        weight = weights[0:1, lanes]
        inv = F32(1.0 / M)
        res_re = jnp.where(alive, weight * (observed[0, 0:1, lanes] - model_re * inv), F32(0.0))
        res_im = jnp.where(alive, weight * (observed[0, 1:2, lanes] - model_im * inv), F32(0.0))
        residual_out[0, 0:1, lanes] = res_re
        residual_out[0, 1:2, lanes] = res_im

    across = (((1,), (1,)), ((), ()))
    swaps = []
    for c in range(parts):
        for i in range(vis // chunk):
            lanes = slice(i * chunk, (i + 1) * chunk)
            r0 = residual_out[0, 0:1, lanes].astype(BF16)
            r1 = residual_out[0, 1:2, lanes].astype(BF16)
            cos_u = du[c * half : (c + 1) * half, lanes]
            sin_u = du[M + c * half : M + (c + 1) * half, lanes]
            spread[c, :half, lanes] = cos_u * r0 - sin_u * r1
            spread[c, half:, lanes] = sin_u * r0 + cos_u * r1
        for i in range(2):
            here = slice(i * M, (i + 1) * M)
            acc[here, :] = lax.dot_general(
                dv[here, :], spread[c], across, preferred_element_type=F32
            )
        acc[:M, :half] = acc[:M, :half] - acc[M:, half:]
        acc[:M, half:] = acc[:M, half:] + acc[M:, :half]
        split(c, s_c, F32((vis * groups) ** (-0.5)))
        swaps.append(swap(4, c, s_c, x_c))
        swaps[c].start()
        if c:
            swaps[c - 1].wait()
            scatter(5, c - 1, s_c, x_c, r_c)

    out_cols = sub * local_cols + lanes_iota(local_cols)
    coarse = unit(column_offset[0] + rows_iota(M // step, step), out_cols, NIMG)
    fine = unit(rows_iota(step), out_cols, NIMG)
    out_norm = F32(M ** (-0.5))

    def put_t6(a, c, s):
        which, at = a * step // half, a * step % half
        t6[which, at : at + step, :] = (c * out_norm).astype(BF16)
        t6[which, half + at : half + at + step, :] = (s * -out_norm).astype(BF16)

    phase_product(coarse, fine, put_t6)
    swaps[-1].wait()
    scatter(5, parts - 1, s_c, x_c, r_c)

    def slab(c, f, count):
        return r_d.at[c, pl.ds(d_slot(parity, f, 0), count)]

    def column_copy(c, k, f, device, arrived):
        piece = r_d.at[c, d_slot(parity, f, spot)]
        return pltpu.make_async_remote_copy(
            piece, piece, d_send.at[0, c, k], d_recv.at[0, c, arrived], device, MESH
        )

    def level_copy(c, f, piece, device):
        return pltpu.make_async_remote_copy(
            piece, piece, d_send.at[1, c, f], d_recv.at[1, c, f], device, MESH
        )

    def level_sends(c, f):
        for device in levels:
            level_copy(c, f, r_d.at[c, d_slot(parity, f, spot)], device).start()

    def level_done(c, f):
        return level_copy(c, f, slab(c, f, plane - 1), sibling)

    def level_relay(c, f):
        whole = slab(c, f, plane)
        return pltpu.make_async_remote_copy(
            whole, whole, d_send.at[2, c, f], d_recv.at[2, c, f], sibling, MESH
        )

    for c in range(parts):
        wait_all(5, c, r_c, half_group - 1)
        r_d[c, d_slot(parity, facet, spot)] = summed(r_c, c)
        for k in range(n_facet - 1, 0, -1):
            device = {"facet": sources[k], "sub": sub, "base": base}
            column_copy(c, k, facet, device, facet).start()
        level_sends(c, facet)
    scale = F32((n_sub * M) ** (-0.5))

    def pass_on(c):
        for k in range(1, n_facet):
            column_copy(c, k, sources[k], sibling, sources[k]).wait_recv()
            level_sends(c, sources[k])

    def land(c, k):
        for f in [sources[k]] if stages > 1 else sources:
            level_done(c, f).wait_recv()
            level_relay(c, f).start()

    def build(c, k):
        for f in [sources[k]] if stages > 1 else sources:
            level_relay(c, f).wait_recv()
        for g, r, col, height, width in pieces(groups, wide)[:half_group]:
            if stages > 1:
                if g >= pairs:
                    continue
                f = sources[k]
            else:
                f = g // pairs
            part = min(width, half)
            for s in range(n_sub):
                for which in range(2):
                    block = r_d[c, d_slot(which, f, s * pairs + g % pairs)]
                    at = 2 * run * k + (2 * s + which) * span + r
                    low = slice(at + run, at + run + height)
                    for inner in range(0, width, part):
                        value = block[:, inner : inner + part]
                        to = col + inner
                        zed[c, at : at + height, to : to + part] = value
                        if to < half:
                            zed[c, low, half + to : half + to + part] = value
                        else:
                            zed[c, low, to - half : to - half + part] = -value

    def take(c, k):
        build(c, k)
        some = slice(2 * run * k, 2 * run * (k + 1))
        for i in range(rows // tile):
            here = slice(i * tile, (i + 1) * tile)
            term = jnp.dot(t5[here, some], zed[c, some], preferred_element_type=F32)
            wave[c, here, :] = wave[c, here, :] + term if k else term

    def finish(c):
        take(c, stages - 1)
        for i in range(rows // tile):
            here = slice(i * tile, (i + 1) * tile)
            share[here, :] = (wave[c, here, :] * scale).astype(BF16)
        for i in range(rows // tile):
            here = slice(i * tile, (i + 1) * tile)
            term = jnp.dot(share[here, :], t6[c], preferred_element_type=F32)
            partial[here, :] = partial[here, :] + term if c else term

    pass_on(0)
    inner = range(1, stages - 1)
    if parts == 2 and stages > 1:
        land(0, 0)
        pass_on(1)
        land(1, 0)
        for k in inner:
            land(0, k)
        take(0, 0)
        take(1, 0)
        land(0, stages - 1)
        for k in inner:
            land(1, k)
        for k in inner:
            take(0, k)
        land(1, stages - 1)
        for k in inner:
            take(1, k)
        finish(0)
        build(1, stages - 1)
    else:
        for c in range(1, parts):
            pass_on(c)
        for c in range(parts):
            for k in range(stages):
                land(c, k)
        for c in range(parts):
            for k in range(stages - 1):
                take(c, k)
            if c + 1 < parts:
                finish(c)
        build(parts - 1, stages - 1)

    for c in range(parts):
        for k in range(n_facet):
            level_done(c, sources[k]).wait_send()
            level_relay(c, sources[k]).wait_send()
            if k:
                column_copy(c, k, facet, sibling, facet).wait_send()


def deliver(
    scale,
    stages,
    residual,
    t5,
    t6,
    zed,
    partial,
    wave,
    residual_out,
    update_out,
    share,
    update,
    sem,
    sems,
):
    first = pltpu.make_async_copy(residual, residual_out, sem)
    first.start()
    rows, depth = t5.shape
    tile = min(256, rows)
    last = zed.shape[0] - 1
    some = slice(depth - depth // stages, depth)
    tiles = [slice(i * tile, (i + 1) * tile) for i in range(rows // tile)]
    writes = []
    for start in range(0, len(tiles), 2):
        for here in tiles[start : start + 2]:
            total = jnp.dot(t5[here, some], zed[last, some], preferred_element_type=F32)
            if stages > 1:
                total = wave[last, here, :] + total
            share[here, :] = (total * F32(scale)).astype(BF16)
        for i, here in list(enumerate(tiles))[start : start + 2]:
            term = jnp.dot(share[here, :], t6[last], preferred_element_type=F32)
            if last:
                term = partial[here, :] + term
            update[here, :] = term.astype(BF16)
            writes.append(
                pltpu.make_async_copy(update.at[here, :], update_out.at[here, :], sems.at[i])
            )
            writes[i].start()
    first.wait()
    for write in writes:
        write.wait()


def shards(
    sizes,
    sky_image,
    facet_rows,
    column_offset,
    subgrid_offsets,
    vis_u,
    vis_v,
    observed,
    weights,
    block_counts,
):
    n_facet, n_sub, n_base = sizes
    groups = n_facet * n_base
    parts = halves(groups)
    wide = 2 * M // parts
    rows, columns = sky_image.shape
    vis = vis_u.shape[1]
    local_cols = columns // n_sub
    _, _, _, height, width = pieces(groups, wide)[0]
    smem = pl.BlockSpec(memory_space=pltpu.SMEM)
    vmem = pl.BlockSpec(memory_space=pltpu.VMEM)
    hbm = pl.BlockSpec(memory_space=pltpu.HBM)
    block = (parts, groups, height, width)
    half_block = (parts, groups // 2, height, width)
    kept = (
        pltpu.VMEM((rows, 2 * M * n_sub), BF16),
        pltpu.VMEM((parts, wide, local_cols), BF16),
        pltpu.VMEM((parts, 2 * M * n_sub, wide), BF16),
        pltpu.VMEM((rows, local_cols), F32),
        pltpu.VMEM((parts, rows, wide), F32),
    )
    room = sum(math.prod(k.shape) * jnp.dtype(k.dtype).itemsize for k in kept)
    results = pl.pallas_call(
        functools.partial(kernel, sizes),
        out_shape=(
            pltpu.VMEM(observed.shape, F32),
            *kept,
        ),
        in_specs=[hbm, smem, hbm, smem] + [hbm] * 5,
        out_specs=(vmem,) * 6,
        scratch_shapes=[
            pltpu.SMEM(facet_rows.shape, jnp.int32),
            pltpu.SMEM(subgrid_offsets.shape, jnp.int32),
            pltpu.VMEM((rows, columns), BF16),
            pltpu.VMEM(vis_u.shape, jnp.int32),
            pltpu.VMEM(vis_v.shape, jnp.int32),
            pltpu.VMEM(observed.shape, F32),
            pltpu.VMEM(weights.shape, F32),
            pltpu.VMEM((parts, columns, wide), BF16),
            pltpu.VMEM((parts, 2 * rows, wide), BF16),
            pltpu.VMEM((M, 2 * rows), BF16),
            pltpu.VMEM((2 * M, vis), BF16),
            pltpu.VMEM((2 * M, vis), BF16),
            pltpu.VMEM((2, M, 2 * M), BF16),
            pltpu.VMEM((2, vis), F32),
            pltpu.VMEM((2 * M, wide), F32),
            pltpu.VMEM((parts, wide, vis), BF16),
            pltpu.VMEM((rows, wide), BF16),
            pltpu.VMEM(block, BF16),
            pltpu.VMEM(half_block, BF16),
            pltpu.VMEM(half_block, BF16),
            pltpu.VMEM(block, BF16),
            pltpu.VMEM(block, BF16),
            pltpu.VMEM(half_block, BF16),
            pltpu.VMEM(half_block, BF16),
            pltpu.VMEM((parts, n_sub * groups, height, width), BF16),
            pltpu.SemaphoreType.DMA((rows // min(256, rows),)),
            pltpu.SemaphoreType.DMA((4,)),
            pltpu.SemaphoreType.DMA((2,)),
            pltpu.SemaphoreType.DMA((6, parts)),
            pltpu.SemaphoreType.DMA((6, parts)),
            pltpu.SemaphoreType.DMA((3, parts, n_facet)),
            pltpu.SemaphoreType.DMA((3, parts, n_facet)),
        ],
        compiler_params=pltpu.CompilerParams(
            collective_id=0, has_side_effects=True, vmem_limit_bytes=61 * 1024 * 1024 - room
        ),
        name="column",
    )(
        facet_rows,
        column_offset,
        subgrid_offsets,
        block_counts,
        sky_image,
        vis_u,
        vis_v,
        observed,
        weights,
    )
    return pl.pallas_call(
        functools.partial(deliver, (n_sub * M) ** (-0.5), layers(n_facet, groups)),
        out_shape=(
            jax.ShapeDtypeStruct(observed.shape, F32),
            jax.ShapeDtypeStruct((rows, local_cols), BF16),
        ),
        in_specs=[vmem] * 6,
        out_specs=(hbm, hbm),
        scratch_shapes=[
            pltpu.VMEM((rows, wide), BF16),
            pltpu.VMEM((rows, local_cols), BF16),
            pltpu.SemaphoreType.DMA,
            pltpu.SemaphoreType.DMA((rows // min(256, rows),)),
        ],
        compiler_params=pltpu.CompilerParams(vmem_limit_bytes=8 * 1024 * 1024),
        name="deliver",
    )(*[pltpu.with_memory_space_constraint(r, pltpu.VMEM) for r in results])


def solution(mesh):
    sizes = (mesh.shape["facet"], mesh.shape["sub"], mesh.shape["base"])
    return jax.shard_map(
        functools.partial(shards, sizes),
        mesh=mesh,
        in_specs=(
            P(("facet", "base"), None),
            P(),
            P(),
            P(),
            P("sub", ("facet", "base")),
            P("sub", ("facet", "base")),
            P("sub", None, ("facet", "base")),
            P("sub", ("facet", "base")),
            P("sub", ("facet", "base")),
        ),
        out_specs=(P("sub", None, ("facet", "base")), P(("facet", "base"), "sub")),
        check_vma=False,
    )
```

```python
import functools
import math

import jax
import jax.numpy as jnp
from jax import lax
from jax.experimental import pallas as pl
from jax.experimental.pallas import tpu as pltpu
from jax.sharding import PartitionSpec as P

NIMG = 131072
M = 256
SUBW = 1024
BLOCK = 128
MESH = pl.DeviceIdType.MESH
F32 = jnp.float32
BF16 = jnp.bfloat16


def unit(first, second, period):
    half = period // 2
    turn = ((first * second + half) & (period - 1)) - half
    y = turn.astype(F32) * (math.pi / period)
    q = y * y
    s = F32(-1.0 / 39916800.0)
    for k in (362880.0, -5040.0, 120.0, -6.0):
        s = s * q + F32(1.0 / k)
    s = (s * q + F32(1.0)) * y
    c = F32(1.0 / 479001600.0)
    for k in (-3628800.0, 40320.0, -720.0, 24.0, -2.0):
        c = c * q + F32(1.0 / k)
    c = c * q + F32(1.0)
    return F32(1.0) - F32(2.0) * s * s, F32(2.0) * s * c


def rows_iota(count, step=1):
    return lax.broadcasted_iota(jnp.int32, (count, 1), 0) * step


def lanes_iota(count):
    return lax.broadcasted_iota(jnp.int32, (1, count), 1)


def phase_product(coarse, fine, put):
    coarse_cos, coarse_sin = coarse
    fine_cos, fine_sin = fine
    for a in range(coarse_cos.shape[0]):
        ca, sa = coarse_cos[a : a + 1, :], coarse_sin[a : a + 1, :]
        put(a, ca * fine_cos - sa * fine_sin, sa * fine_cos + ca * fine_sin)


def pieces(groups, cols):
    row_blocks = min(groups, M // 16)
    col_blocks = groups // row_blocks
    height, width = M // row_blocks, cols // col_blocks
    return [
        (r * col_blocks + c, r * height, c * width, height, width)
        for r in range(row_blocks)
        for c in range(col_blocks)
    ]


def halves(groups):
    return 2 if groups <= M // 16 else 1


def layers(n_facet, groups):
    return n_facet if groups <= M // 16 else 1


def far_first(count):
    return sorted(range(1, count), key=lambda j: (-min(j, count - j), j))


def kernel(
    sizes,
    facet_rows_hbm,
    column_offset,
    subgrid_offsets_hbm,
    counts,
    sky_hbm,
    vis_u_hbm,
    vis_v_hbm,
    observed_hbm,
    weights_hbm,
    residual_out,
    t5,
    t6,
    zed,
    partial,
    wave,
    facet_rows,
    subgrid_offsets,
    sky,
    vis_u,
    vis_v,
    observed,
    weights,
    t1,
    spec,
    t2,
    du,
    dv,
    lhs,
    model,
    acc,
    spread,
    share,
    s_a,
    x_a,
    r_a,
    r_b,
    s_c,
    x_c,
    r_c,
    r_d,
    sky_sem,
    side_sem,
    small_sem,
    send_sem,
    recv_sem,
    d_send,
    d_recv,
):
    n_facet, n_sub, n_base = sizes
    groups = n_facet * n_base
    parts = halves(groups)
    wide = 2 * M // parts
    half = wide // 2
    stages = layers(n_facet, groups)
    rows, columns = sky.shape
    tile = min(256, rows)
    vis = vis_u.shape[1]
    local_cols = t6.shape[2]
    facet, sub, base = lax.axis_index("facet"), lax.axis_index("sub"), lax.axis_index("base")
    pairs = n_base // 2
    half_group = groups // 2
    plane = n_sub * pairs
    parity = lax.rem(base, 2)
    row_of_base = base // 2
    pair = facet * pairs + row_of_base
    spot = sub * pairs + row_of_base
    sibling = {"facet": facet, "sub": sub, "base": base + 1 - 2 * parity}

    def d_slot(which, f, place):
        return (which * n_facet + f) * plane + place

    def by_distance(k):
        edge = lax.min(facet, n_facet - 1 - facet)
        across = facet + (k + 1) // 2 * (1 - k % 2 * 2)
        beyond = jnp.where(2 * facet < n_facet, k, n_facet - 1 - k)
        return jnp.where(k <= 2 * edge, across, beyond)

    sources = [facet] + [by_distance(k) for k in range(1, n_facet)]
    mates = [
        (f * pairs + q, {"facet": f, "sub": sub, "base": q * 2 + parity})
        for f in sources[:0:-1]
        for q in [lax.rem(row_of_base + d, pairs) for d in range(pairs)[::-1]]
    ] + [
        (facet * pairs + q, {"facet": facet, "sub": sub, "base": q * 2 + parity})
        for q in [lax.rem(row_of_base + d, pairs) for d in range(1, pairs)]
    ]
    steps = [(a, b) for a in range(n_sub) for b in range(pairs)][1:]
    steps.sort(key=lambda ab: (not (ab[0] and ab[1]), bool(ab[0])))
    levels = [
        {
            "facet": facet,
            "sub": lax.rem(sub + a, n_sub),
            "base": lax.rem(row_of_base + b, pairs) * 2 + parity,
        }
        for a, b in steps
    ]

    smalls = [
        pltpu.make_async_copy(source, target, small_sem.at[i])
        for i, (source, target) in enumerate(
            (
                (facet_rows_hbm, facet_rows),
                (subgrid_offsets_hbm, subgrid_offsets),
            )
        )
    ]
    for small in smalls:
        small.start()
    fetches = []
    for i in range(rows // tile):
        here = pl.ds(i * tile, tile)
        fetches.append(
            pltpu.make_async_copy(sky_hbm.at[here, :], sky.at[here, :], sky_sem.at[i])
        )
        fetches[i].start()
    sides = [
        pltpu.make_async_copy(source, target, side_sem.at[i])
        for i, (source, target) in enumerate(
            (
                (vis_u_hbm, vis_u),
                (vis_v_hbm, vis_v),
                (observed_hbm, observed),
                (weights_hbm, weights),
            )
        )
    ]
    for side in sides:
        side.start()
    barrier = pltpu.get_barrier_semaphore()

    def greet(device):
        pl.semaphore_signal(barrier, inc=1, device_id=device, device_id_type=MESH)

    greet(sibling)
    for _, device in mates:
        greet(device)
    for j in range((n_sub - 1) * pairs):
        other = lax.rem(sub + 1 + j // pairs, n_sub)
        greet({"facet": facet, "sub": other, "base": j % pairs * 2 + parity})
    partners = 1 + (half_group - 1) + (n_sub - 1) * pairs

    def wait_all(phase, c, buffer, count):
        whole = buffer.at[c, pl.ds(0, count)]
        done = pltpu.make_async_remote_copy(
            whole, whole, send_sem.at[phase, c], recv_sem.at[phase, c], sibling, MESH
        )
        done.wait_recv()
        done.wait_send()

    def swap(phase, c, source, extra):
        theirs = source.at[c, pl.ds((1 - parity) * half_group, half_group)]
        return pltpu.make_async_remote_copy(
            theirs,
            extra.at[c],
            send_sem.at[phase, c],
            recv_sem.at[phase, c],
            sibling,
            MESH,
        )

    def scatter(phase, c, source, extra, landing):
        for i in range(half_group):
            at = parity * half_group + i
            joint = source[c, at].astype(F32) + extra[c, i].astype(F32)
            source[c, at] = joint.astype(BF16)

        for other, device in mates:
            pltpu.make_async_remote_copy(
                source.at[c, parity * half_group + other],
                landing.at[c, pair],
                send_sem.at[phase, c],
                recv_sem.at[phase, c],
                device,
                MESH,
            ).start()
        landing[c, pair] = source[c, parity * half_group + pair]

    def summed(landing, c):
        result = landing[c, 0].astype(F32)
        for g in range(1, half_group):
            result = result + landing[c, g].astype(F32)
        return result.astype(BF16)

    def gather(phase, c, buffer):
        slot = parity * half_group + pair

        for _, device in mates:
            pltpu.make_async_remote_copy(
                buffer.at[c, slot],
                buffer.at[c, slot],
                send_sem.at[phase, c],
                recv_sem.at[phase, c],
                device,
                MESH,
            ).start()

    def relay(phase, c, buffer):
        mine = buffer.at[c, pl.ds(parity * half_group, half_group)]
        return pltpu.make_async_remote_copy(
            mine, mine, send_sem.at[phase, c], recv_sem.at[phase, c], sibling, MESH
        )

    def split(c, target, scale):
        for g, r, k, height, width in pieces(groups, wide):
            target[c, g] = (acc[r : r + height, k : k + width] * scale).astype(BF16)

    high = 128
    fan = 16
    step = 32
    freq = column_offset[0] + lanes_iota(M)
    coarse_1 = unit(rows_iota(columns // step, step), freq, NIMG)
    fine_1 = unit(rows_iota(step), freq, NIMG)
    norm = F32(columns ** (-0.5))

    def make_t1(c):
        lanes = slice(c * half, (c + 1) * half)

        def put(a, cosine, sine):
            t1[c, a * step : (a + 1) * step, :half] = (cosine * norm).astype(BF16)
            t1[c, a * step : (a + 1) * step, half:] = (sine * -norm).astype(BF16)

        phase_product([x[:, lanes] for x in coarse_1], [x[:, lanes] for x in fine_1], put)

    def make_spec(c):
        for i in range(rows // tile):
            here = slice(i * tile, (i + 1) * tile)
            there = slice(rows + i * tile, rows + (i + 1) * tile)
            if not c and not i % 2:
                for later in fetches[i : i + 2]:
                    later.wait()
            part = jnp.dot(sky[here, :], t1[c], preferred_element_type=F32)
            real, imag = part[:, :half].astype(BF16), part[:, half:].astype(BF16)
            spec[c, here, :half] = real
            spec[c, here, half:] = imag
            spec[c, there, :half] = imag
            spec[c, there, half:] = -real

    def contribution(c):
        for i in range(2):
            here = slice(i * M // 2, (i + 1) * M // 2)
            acc[here, :] = jnp.dot(t2[here, :], spec[c], preferred_element_type=F32)
        split(c, s_a, F32((rows * groups) ** (-0.5)))


    def grid_table(position, table):
        width = 512
        for at in range(0, vis, width):
            lanes = slice(at, at + width)
            place = position[0:1, lanes]
            coarse = unit(rows_iota(M // fan, fan), place, SUBW)
            fine = unit(rows_iota(fan), place, SUBW)

            def put(a, c, s):
                table[a * fan : (a + 1) * fan, lanes] = c.astype(BF16)
                table[M + a * fan : M + (a + 1) * fan, lanes] = s.astype(BF16)

            phase_product(coarse, fine, put)

    for c in range(parts):
        make_t1(c)
    for small in smalls:
        small.wait()
    row_start = facet_rows[facet] + base * rows
    positions = row_start + lanes_iota(rows)
    own_offset = subgrid_offsets[sub]
    coarse_2 = unit(own_offset + rows_iota(M // fan, fan), positions, NIMG)
    fine_2 = unit(rows_iota(fan), positions, NIMG)

    def put_t2(a, c, s):
        t2[a * fan : (a + 1) * fan, :rows] = c.astype(BF16)
        t2[a * fan : (a + 1) * fan, rows:] = s.astype(BF16)

    phase_product(coarse_2, fine_2, put_t2)

    swaps = []
    for c in range(parts):
        make_spec(c)
        contribution(c)
        if not c:
            pl.semaphore_wait(barrier, partners)
        swaps.append(swap(0, c, s_a, x_a))
        swaps[c].start()
        if c:
            swaps[c - 1].wait()
            scatter(1, c - 1, s_a, x_a, r_a)
    for side in sides:
        side.wait()
    grid_table(vis_u, du)
    swaps[-1].wait()
    scatter(1, parts - 1, s_a, x_a, r_a)
    grid_table(vis_v, dv)
    for c in range(parts):
        wait_all(1, c, r_a, half_group - 1)
        r_b[c, parity * half_group + pair] = summed(r_a, c)
        gather(2, c, r_b)

    span = M // 2 // stages
    run = n_sub * 2 * span
    lane = lanes_iota(run)
    start = lax.rem(lane // span, 2) * (M // 2) + lax.rem(lane, span)
    for s in range(n_sub):
        start = start + jnp.where(lane // (2 * span) == s, subgrid_offsets[s], 0)
    for k in range(stages):
        freqs = start + sources[k] * span if stages > 1 else start
        coarse = unit(row_start + rows_iota(rows // high, high), freqs, NIMG)
        fine = unit(rows_iota(high), freqs, NIMG)

        def put_t5(a, c, sine, at=2 * run * k):
            t5[a * high : (a + 1) * high, at : at + run] = c.astype(BF16)
            t5[a * high : (a + 1) * high, at + run : at + 2 * run] = sine.astype(BF16)

        phase_product(coarse, fine, put_t5)

    relays = []
    for c in range(parts):
        wait_all(2, c, r_b, half_group - 1)
        relays.append(relay(3, c, r_b))
        relays[c].start()

    top = M // 2

    def make_lhs(which, c):
        for g, r, k, height, width in pieces(groups, wide)[:half_group]:
            block = r_b[c, which * half_group + g]
            part = min(width, half)
            for inner in range(0, width, part):
                value = block[:, inner : inner + part]
                at = k + inner
                if at < half:
                    re = c * half + at
                    lhs[which, r : r + height, re : re + part] = value
                    lhs[which, top + r : top + r + height, M + re : M + re + part] = -value
                else:
                    im = c * half + at - half
                    lhs[which, r : r + height, M + im : M + im + part] = value
                    lhs[which, top + r : top + r + height, im : im + part] = value

    chunk = 512
    live = counts[0, 0] * BLOCK

    def model_terms(which, lanes):
        both = jnp.dot(lhs[which], du[:, lanes], preferred_element_type=F32)
        both_re, both_im = both[:top], both[top:]
        cos_v = dv[pl.ds(pl.multiple_of(which * top, top), top), lanes].astype(F32)
        sin_v = dv[pl.ds(pl.multiple_of(M + which * top, top), top), lanes].astype(F32)
        return (
            jnp.sum(cos_v * both_re + sin_v * both_im, axis=0, keepdims=True),
            jnp.sum(cos_v * both_im - sin_v * both_re, axis=0, keepdims=True),
        )

    for c in range(parts):
        make_lhs(parity, c)
    for i in range(vis // chunk):
        lanes = slice(i * chunk, (i + 1) * chunk)
        model[0:1, lanes], model[1:2, lanes] = model_terms(parity, lanes)
    for c in range(parts):
        relays[c].wait()
    for c in range(parts):
        make_lhs(1 - parity, c)
    for i in range(vis // chunk):
        lanes = slice(i * chunk, (i + 1) * chunk)
        model_re, model_im = model_terms(1 - parity, lanes)
        model_re, model_im = model_re + model[0:1, lanes], model_im + model[1:2, lanes]
        alive = lanes_iota(chunk) + i * chunk < live
        weight = weights[0:1, lanes]
        inv = F32(1.0 / M)
        res_re = jnp.where(alive, weight * (observed[0, 0:1, lanes] - model_re * inv), F32(0.0))
        res_im = jnp.where(alive, weight * (observed[0, 1:2, lanes] - model_im * inv), F32(0.0))
        residual_out[0, 0:1, lanes] = res_re
        residual_out[0, 1:2, lanes] = res_im

    across = (((1,), (1,)), ((), ()))
    swaps = []
    for c in range(parts):
        for i in range(vis // chunk):
            lanes = slice(i * chunk, (i + 1) * chunk)
            r0 = residual_out[0, 0:1, lanes].astype(BF16)
            r1 = residual_out[0, 1:2, lanes].astype(BF16)
            cos_u = du[c * half : (c + 1) * half, lanes]
            sin_u = du[M + c * half : M + (c + 1) * half, lanes]
            spread[c, :half, lanes] = cos_u * r0 - sin_u * r1
            spread[c, half:, lanes] = sin_u * r0 + cos_u * r1
        for i in range(2):
            here = slice(i * M, (i + 1) * M)
            acc[here, :] = lax.dot_general(
                dv[here, :], spread[c], across, preferred_element_type=F32
            )
        acc[:M, :half] = acc[:M, :half] - acc[M:, half:]
        acc[:M, half:] = acc[:M, half:] + acc[M:, :half]
        split(c, s_c, F32((vis * groups) ** (-0.5)))
        swaps.append(swap(4, c, s_c, x_c))
        swaps[c].start()
        if c:
            swaps[c - 1].wait()
            scatter(5, c - 1, s_c, x_c, r_c)

    out_cols = sub * local_cols + lanes_iota(local_cols)
    coarse = unit(column_offset[0] + rows_iota(M // step, step), out_cols, NIMG)
    fine = unit(rows_iota(step), out_cols, NIMG)
    out_norm = F32(M ** (-0.5))

    def put_t6(a, c, s):
        which, at = a * step // half, a * step % half
        t6[which, at : at + step, :] = (c * out_norm).astype(BF16)
        t6[which, half + at : half + at + step, :] = (s * -out_norm).astype(BF16)

    phase_product(coarse, fine, put_t6)
    swaps[-1].wait()
    scatter(5, parts - 1, s_c, x_c, r_c)

    def slab(c, f, count):
        return r_d.at[c, pl.ds(d_slot(parity, f, 0), count)]

    def column_copy(c, k, f, device, arrived):
        piece = r_d.at[c, d_slot(parity, f, spot)]
        return pltpu.make_async_remote_copy(
            piece, piece, d_send.at[0, c, k], d_recv.at[0, c, arrived], device, MESH
        )

    def level_copy(c, f, piece, device):
        return pltpu.make_async_remote_copy(
            piece, piece, d_send.at[1, c, f], d_recv.at[1, c, f], device, MESH
        )

    def level_sends(c, f):
        for device in levels:
            level_copy(c, f, r_d.at[c, d_slot(parity, f, spot)], device).start()

    def level_done(c, f):
        return level_copy(c, f, slab(c, f, plane - 1), sibling)

    def level_relay(c, f):
        whole = slab(c, f, plane)
        return pltpu.make_async_remote_copy(
            whole, whole, d_send.at[2, c, f], d_recv.at[2, c, f], sibling, MESH
        )

    for c in range(parts):
        wait_all(5, c, r_c, half_group - 1)
        r_d[c, d_slot(parity, facet, spot)] = summed(r_c, c)
        for k in range(n_facet - 1, 0, -1):
            device = {"facet": sources[k], "sub": sub, "base": base}
            column_copy(c, k, facet, device, facet).start()
        level_sends(c, facet)
    scale = F32((n_sub * M) ** (-0.5))

    def pass_on(c):
        for k in range(1, n_facet):
            column_copy(c, k, sources[k], sibling, sources[k]).wait_recv()
            level_sends(c, sources[k])

    def land(c, k):
        for f in [sources[k]] if stages > 1 else sources:
            level_done(c, f).wait_recv()
            level_relay(c, f).start()

    def build(c, k):
        for f in [sources[k]] if stages > 1 else sources:
            level_relay(c, f).wait_recv()
        for g, r, col, height, width in pieces(groups, wide)[:half_group]:
            if stages > 1:
                if g >= pairs:
                    continue
                f = sources[k]
            else:
                f = g // pairs
            part = min(width, half)
            for s in range(n_sub):
                for which in range(2):
                    block = r_d[c, d_slot(which, f, s * pairs + g % pairs)]
                    at = 2 * run * k + (2 * s + which) * span + r
                    low = slice(at + run, at + run + height)
                    for inner in range(0, width, part):
                        value = block[:, inner : inner + part]
                        to = col + inner
                        zed[c, at : at + height, to : to + part] = value
                        if to < half:
                            zed[c, low, half + to : half + to + part] = value
                        else:
                            zed[c, low, to - half : to - half + part] = -value

    def take(c, k):
        build(c, k)
        some = slice(2 * run * k, 2 * run * (k + 1))
        for i in range(rows // tile):
            here = slice(i * tile, (i + 1) * tile)
            term = jnp.dot(t5[here, some], zed[c, some], preferred_element_type=F32)
            wave[c, here, :] = wave[c, here, :] + term if k else term

    def finish(c):
        take(c, stages - 1)
        for i in range(rows // tile):
            here = slice(i * tile, (i + 1) * tile)
            share[here, :] = (wave[c, here, :] * scale).astype(BF16)
        for i in range(rows // tile):
            here = slice(i * tile, (i + 1) * tile)
            term = jnp.dot(share[here, :], t6[c], preferred_element_type=F32)
            partial[here, :] = partial[here, :] + term if c else term

    pass_on(0)
    inner = range(1, stages - 1)
    if parts == 2 and stages > 1:
        land(0, 0)
        pass_on(1)
        land(1, 0)
        for k in inner:
            land(0, k)
        take(0, 0)
        take(1, 0)
        land(0, stages - 1)
        for k in inner:
            land(1, k)
        for k in inner:
            take(0, k)
        land(1, stages - 1)
        for k in inner:
            take(1, k)
        finish(0)
        build(1, stages - 1)
    else:
        for c in range(1, parts):
            pass_on(c)
        for c in range(parts):
            for k in range(stages):
                land(c, k)
        for c in range(parts):
            for k in range(stages - 1):
                take(c, k)
            if c + 1 < parts:
                finish(c)
        build(parts - 1, stages - 1)

    for c in range(parts):
        for k in range(n_facet):
            level_done(c, sources[k]).wait_send()
            level_relay(c, sources[k]).wait_send()
            if k:
                column_copy(c, k, facet, sibling, facet).wait_send()


def deliver(
    scale,
    stages,
    residual,
    t5,
    t6,
    zed,
    partial,
    wave,
    residual_out,
    update_out,
    share,
    update,
    sem,
    sems,
):
    first = pltpu.make_async_copy(residual, residual_out, sem)
    first.start()
    rows, depth = t5.shape
    tile = min(512, rows)
    last = zed.shape[0] - 1
    some = slice(depth - depth // stages, depth)
    tiles = [slice(i * tile, (i + 1) * tile) for i in range(rows // tile)]
    writes = []
    for start in range(0, len(tiles), 2):
        for here in tiles[start : start + 2]:
            total = jnp.dot(t5[here, some], zed[last, some], preferred_element_type=F32)
            if stages > 1:
                total = wave[last, here, :] + total
            share[here, :] = (total * F32(scale)).astype(BF16)
        for i, here in list(enumerate(tiles))[start : start + 2]:
            term = jnp.dot(share[here, :], t6[last], preferred_element_type=F32)
            if last:
                term = partial[here, :] + term
            update[here, :] = term.astype(BF16)
            writes.append(
                pltpu.make_async_copy(update.at[here, :], update_out.at[here, :], sems.at[i])
            )
            writes[i].start()
    first.wait()
    for write in writes:
        write.wait()


def shards(
    sizes,
    sky_image,
    facet_rows,
    column_offset,
    subgrid_offsets,
    vis_u,
    vis_v,
    observed,
    weights,
    block_counts,
):
    n_facet, n_sub, n_base = sizes
    groups = n_facet * n_base
    parts = halves(groups)
    wide = 2 * M // parts
    rows, columns = sky_image.shape
    vis = vis_u.shape[1]
    local_cols = columns // n_sub
    _, _, _, height, width = pieces(groups, wide)[0]
    smem = pl.BlockSpec(memory_space=pltpu.SMEM)
    vmem = pl.BlockSpec(memory_space=pltpu.VMEM)
    hbm = pl.BlockSpec(memory_space=pltpu.HBM)
    block = (parts, groups, height, width)
    half_block = (parts, groups // 2, height, width)
    kept = (
        pltpu.VMEM((rows, 2 * M * n_sub), BF16),
        pltpu.VMEM((parts, wide, local_cols), BF16),
        pltpu.VMEM((parts, 2 * M * n_sub, wide), BF16),
        pltpu.VMEM((rows, local_cols), F32),
        pltpu.VMEM((parts, rows, wide), F32),
    )
    room = sum(math.prod(k.shape) * jnp.dtype(k.dtype).itemsize for k in kept)
    results = pl.pallas_call(
        functools.partial(kernel, sizes),
        out_shape=(
            pltpu.VMEM(observed.shape, F32),
            *kept,
        ),
        in_specs=[hbm, smem, hbm, smem] + [hbm] * 5,
        out_specs=(vmem,) * 6,
        scratch_shapes=[
            pltpu.SMEM(facet_rows.shape, jnp.int32),
            pltpu.SMEM(subgrid_offsets.shape, jnp.int32),
            pltpu.VMEM((rows, columns), BF16),
            pltpu.VMEM(vis_u.shape, jnp.int32),
            pltpu.VMEM(vis_v.shape, jnp.int32),
            pltpu.VMEM(observed.shape, F32),
            pltpu.VMEM(weights.shape, F32),
            pltpu.VMEM((parts, columns, wide), BF16),
            pltpu.VMEM((parts, 2 * rows, wide), BF16),
            pltpu.VMEM((M, 2 * rows), BF16),
            pltpu.VMEM((2 * M, vis), BF16),
            pltpu.VMEM((2 * M, vis), BF16),
            pltpu.VMEM((2, M, 2 * M), BF16),
            pltpu.VMEM((2, vis), F32),
            pltpu.VMEM((2 * M, wide), F32),
            pltpu.VMEM((parts, wide, vis), BF16),
            pltpu.VMEM((rows, wide), BF16),
            pltpu.VMEM(block, BF16),
            pltpu.VMEM(half_block, BF16),
            pltpu.VMEM(half_block, BF16),
            pltpu.VMEM(block, BF16),
            pltpu.VMEM(block, BF16),
            pltpu.VMEM(half_block, BF16),
            pltpu.VMEM(half_block, BF16),
            pltpu.VMEM((parts, n_sub * groups, height, width), BF16),
            pltpu.SemaphoreType.DMA((rows // min(256, rows),)),
            pltpu.SemaphoreType.DMA((4,)),
            pltpu.SemaphoreType.DMA((2,)),
            pltpu.SemaphoreType.DMA((6, parts)),
            pltpu.SemaphoreType.DMA((6, parts)),
            pltpu.SemaphoreType.DMA((3, parts, n_facet)),
            pltpu.SemaphoreType.DMA((3, parts, n_facet)),
        ],
        compiler_params=pltpu.CompilerParams(
            collective_id=0, has_side_effects=True, vmem_limit_bytes=61 * 1024 * 1024 - room
        ),
        name="column",
    )(
        facet_rows,
        column_offset,
        subgrid_offsets,
        block_counts,
        sky_image,
        vis_u,
        vis_v,
        observed,
        weights,
    )
    return pl.pallas_call(
        functools.partial(deliver, (n_sub * M) ** (-0.5), layers(n_facet, groups)),
        out_shape=(
            jax.ShapeDtypeStruct(observed.shape, F32),
            jax.ShapeDtypeStruct((rows, local_cols), BF16),
        ),
        in_specs=[vmem] * 6,
        out_specs=(hbm, hbm),
        scratch_shapes=[
            pltpu.VMEM((rows, wide), BF16),
            pltpu.VMEM((rows, local_cols), BF16),
            pltpu.SemaphoreType.DMA,
            pltpu.SemaphoreType.DMA((rows // min(512, rows),)),
        ],
        compiler_params=pltpu.CompilerParams(vmem_limit_bytes=8 * 1024 * 1024),
        name="deliver",
    )(*[pltpu.with_memory_space_constraint(r, pltpu.VMEM) for r in results])


def solution(mesh):
    sizes = (mesh.shape["facet"], mesh.shape["sub"], mesh.shape["base"])
    return jax.shard_map(
        functools.partial(shards, sizes),
        mesh=mesh,
        in_specs=(
            P(("facet", "base"), None),
            P(),
            P(),
            P(),
            P("sub", ("facet", "base")),
            P("sub", ("facet", "base")),
            P("sub", None, ("facet", "base")),
            P("sub", ("facet", "base")),
            P("sub", ("facet", "base")),
        ),
        out_specs=(P("sub", None, ("facet", "base")), P(("facet", "base"), "sub")),
        check_vma=False,
    )
```

```python
import functools
import math

import jax
import jax.numpy as jnp
from jax import lax
from jax.experimental import pallas as pl
from jax.experimental.pallas import tpu as pltpu
from jax.sharding import PartitionSpec as P

NIMG = 131072
M = 256
SUBW = 1024
BLOCK = 128
MESH = pl.DeviceIdType.MESH
F32 = jnp.float32
BF16 = jnp.bfloat16


def unit(first, second, period):
    half = period // 2
    turn = ((first * second + half) & (period - 1)) - half
    y = turn.astype(F32) * (math.pi / period)
    q = y * y
    s = F32(-1.0 / 39916800.0)
    for k in (362880.0, -5040.0, 120.0, -6.0):
        s = s * q + F32(1.0 / k)
    s = (s * q + F32(1.0)) * y
    c = F32(1.0 / 479001600.0)
    for k in (-3628800.0, 40320.0, -720.0, 24.0, -2.0):
        c = c * q + F32(1.0 / k)
    c = c * q + F32(1.0)
    return F32(1.0) - F32(2.0) * s * s, F32(2.0) * s * c


def rows_iota(count, step=1):
    return lax.broadcasted_iota(jnp.int32, (count, 1), 0) * step


def lanes_iota(count):
    return lax.broadcasted_iota(jnp.int32, (1, count), 1)


def phase_product(coarse, fine, put):
    coarse_cos, coarse_sin = coarse
    fine_cos, fine_sin = fine
    for a in range(coarse_cos.shape[0]):
        ca, sa = coarse_cos[a : a + 1, :], coarse_sin[a : a + 1, :]
        put(a, ca * fine_cos - sa * fine_sin, sa * fine_cos + ca * fine_sin)


def pieces(groups, cols):
    row_blocks = min(groups, M // 16)
    col_blocks = groups // row_blocks
    height, width = M // row_blocks, cols // col_blocks
    return [
        (r * col_blocks + c, r * height, c * width, height, width)
        for r in range(row_blocks)
        for c in range(col_blocks)
    ]


def halves(groups):
    return 2 if groups <= M // 16 else 1


def layers(n_facet, groups):
    return n_facet if groups <= M // 16 else 1


def far_first(count):
    return sorted(range(1, count), key=lambda j: (-min(j, count - j), j))


def kernel(
    sizes,
    facet_rows_hbm,
    column_offset,
    subgrid_offsets_hbm,
    counts,
    sky_hbm,
    vis_u_hbm,
    vis_v_hbm,
    observed_hbm,
    weights_hbm,
    residual_out,
    t5,
    t6,
    zed,
    partial,
    wave,
    facet_rows,
    subgrid_offsets,
    sky,
    vis_u,
    vis_v,
    observed,
    weights,
    t1,
    spec,
    t2,
    du,
    dv,
    lhs,
    model,
    acc,
    spread,
    share,
    s_a,
    x_a,
    r_a,
    r_b,
    s_c,
    x_c,
    r_c,
    r_d,
    sky_sem,
    side_sem,
    small_sem,
    send_sem,
    recv_sem,
    d_send,
    d_recv,
):
    n_facet, n_sub, n_base = sizes
    groups = n_facet * n_base
    parts = halves(groups)
    wide = 2 * M // parts
    half = wide // 2
    stages = layers(n_facet, groups)
    rows, columns = sky.shape
    tile = min(256, rows)
    vis = vis_u.shape[1]
    local_cols = t6.shape[2]
    facet, sub, base = lax.axis_index("facet"), lax.axis_index("sub"), lax.axis_index("base")
    pairs = n_base // 2
    half_group = groups // 2
    plane = n_sub * pairs
    parity = lax.rem(base, 2)
    row_of_base = base // 2
    pair = facet * pairs + row_of_base
    spot = sub * pairs + row_of_base
    sibling = {"facet": facet, "sub": sub, "base": base + 1 - 2 * parity}

    def d_slot(which, f, place):
        return (which * n_facet + f) * plane + place

    def by_distance(k):
        edge = lax.min(facet, n_facet - 1 - facet)
        across = facet + (k + 1) // 2 * (1 - k % 2 * 2)
        beyond = jnp.where(2 * facet < n_facet, k, n_facet - 1 - k)
        return jnp.where(k <= 2 * edge, across, beyond)

    sources = [facet] + [by_distance(k) for k in range(1, n_facet)]
    mates = [
        (f * pairs + q, {"facet": f, "sub": sub, "base": q * 2 + parity})
        for f in sources[:0:-1]
        for q in [lax.rem(row_of_base + d, pairs) for d in range(pairs)[::-1]]
    ] + [
        (facet * pairs + q, {"facet": facet, "sub": sub, "base": q * 2 + parity})
        for q in [lax.rem(row_of_base + d, pairs) for d in range(1, pairs)]
    ]
    steps = [(a, b) for a in range(n_sub) for b in range(pairs)][1:]
    steps.sort(key=lambda ab: (not (ab[0] and ab[1]), bool(ab[0])))
    levels = [
        {
            "facet": facet,
            "sub": lax.rem(sub + a, n_sub),
            "base": lax.rem(row_of_base + b, pairs) * 2 + parity,
        }
        for a, b in steps
    ]

    smalls = [
        pltpu.make_async_copy(source, target, small_sem.at[i])
        for i, (source, target) in enumerate(
            (
                (facet_rows_hbm, facet_rows),
                (subgrid_offsets_hbm, subgrid_offsets),
            )
        )
    ]
    for small in smalls:
        small.start()
    fetches = []
    for i in range(rows // tile):
        here = pl.ds(i * tile, tile)
        fetches.append(
            pltpu.make_async_copy(sky_hbm.at[here, :], sky.at[here, :], sky_sem.at[i])
        )
        fetches[i].start()
    sides = [
        pltpu.make_async_copy(source, target, side_sem.at[i])
        for i, (source, target) in enumerate(
            (
                (vis_u_hbm, vis_u),
                (vis_v_hbm, vis_v),
                (observed_hbm, observed),
                (weights_hbm, weights),
            )
        )
    ]
    for side in sides:
        side.start()
    barrier = pltpu.get_barrier_semaphore()

    def greet(device):
        pl.semaphore_signal(barrier, inc=1, device_id=device, device_id_type=MESH)

    greet(sibling)
    for _, device in mates:
        greet(device)
    for j in range((n_sub - 1) * pairs):
        other = lax.rem(sub + 1 + j // pairs, n_sub)
        greet({"facet": facet, "sub": other, "base": j % pairs * 2 + parity})
    partners = 1 + (half_group - 1) + (n_sub - 1) * pairs

    def wait_all(phase, c, buffer, count):
        whole = buffer.at[c, pl.ds(0, count)]
        done = pltpu.make_async_remote_copy(
            whole, whole, send_sem.at[phase, c], recv_sem.at[phase, c], sibling, MESH
        )
        done.wait_recv()
        done.wait_send()

    def swap(phase, c, source, extra):
        theirs = source.at[c, pl.ds((1 - parity) * half_group, half_group)]
        return pltpu.make_async_remote_copy(
            theirs,
            extra.at[c],
            send_sem.at[phase, c],
            recv_sem.at[phase, c],
            sibling,
            MESH,
        )

    def scatter(phase, c, source, extra, landing):
        for i in range(half_group):
            at = parity * half_group + i
            joint = source[c, at].astype(F32) + extra[c, i].astype(F32)
            source[c, at] = joint.astype(BF16)

        for other, device in mates:
            pltpu.make_async_remote_copy(
                source.at[c, parity * half_group + other],
                landing.at[c, pair],
                send_sem.at[phase, c],
                recv_sem.at[phase, c],
                device,
                MESH,
            ).start()
        landing[c, pair] = source[c, parity * half_group + pair]

    def summed(landing, c):
        result = landing[c, 0].astype(F32)
        for g in range(1, half_group):
            result = result + landing[c, g].astype(F32)
        return result.astype(BF16)

    def gather(phase, c, buffer):
        slot = parity * half_group + pair

        for _, device in mates:
            pltpu.make_async_remote_copy(
                buffer.at[c, slot],
                buffer.at[c, slot],
                send_sem.at[phase, c],
                recv_sem.at[phase, c],
                device,
                MESH,
            ).start()

    def relay(phase, c, buffer):
        mine = buffer.at[c, pl.ds(parity * half_group, half_group)]
        return pltpu.make_async_remote_copy(
            mine, mine, send_sem.at[phase, c], recv_sem.at[phase, c], sibling, MESH
        )

    def split(c, target, scale):
        for g, r, k, height, width in pieces(groups, wide):
            target[c, g] = (acc[r : r + height, k : k + width] * scale).astype(BF16)

    high = 128
    fan = 16
    step = 32
    freq = column_offset[0] + lanes_iota(M)
    coarse_1 = unit(rows_iota(columns // step, step), freq, NIMG)
    fine_1 = unit(rows_iota(step), freq, NIMG)
    norm = F32(columns ** (-0.5))

    def make_t1(c):
        lanes = slice(c * half, (c + 1) * half)

        def put(a, cosine, sine):
            t1[c, a * step : (a + 1) * step, :half] = (cosine * norm).astype(BF16)
            t1[c, a * step : (a + 1) * step, half:] = (sine * -norm).astype(BF16)

        phase_product([x[:, lanes] for x in coarse_1], [x[:, lanes] for x in fine_1], put)

    def make_spec(c):
        for i in range(rows // tile):
            here = slice(i * tile, (i + 1) * tile)
            there = slice(rows + i * tile, rows + (i + 1) * tile)
            if not c and not i % 2:
                for later in fetches[i : i + 2]:
                    later.wait()
            part = jnp.dot(sky[here, :], t1[c], preferred_element_type=F32)
            real, imag = part[:, :half].astype(BF16), part[:, half:].astype(BF16)
            spec[c, here, :half] = real
            spec[c, here, half:] = imag
            spec[c, there, :half] = imag
            spec[c, there, half:] = -real

    def contribution(c):
        for i in range(2):
            here = slice(i * M // 2, (i + 1) * M // 2)
            acc[here, :] = jnp.dot(t2[here, :], spec[c], preferred_element_type=F32)
        split(c, s_a, F32((rows * groups) ** (-0.5)))


    def grid_table(position, table):
        width = 512
        for at in range(0, vis, width):
            lanes = slice(at, at + width)
            place = position[0:1, lanes]
            coarse = unit(rows_iota(M // fan, fan), place, SUBW)
            fine = unit(rows_iota(fan), place, SUBW)

            def put(a, c, s):
                table[a * fan : (a + 1) * fan, lanes] = c.astype(BF16)
                table[M + a * fan : M + (a + 1) * fan, lanes] = s.astype(BF16)

            phase_product(coarse, fine, put)

    for c in range(parts):
        make_t1(c)
    for small in smalls:
        small.wait()
    row_start = facet_rows[facet] + base * rows
    positions = row_start + lanes_iota(rows)
    own_offset = subgrid_offsets[sub]
    coarse_2 = unit(own_offset + rows_iota(M // fan, fan), positions, NIMG)
    fine_2 = unit(rows_iota(fan), positions, NIMG)

    def put_t2(a, c, s):
        t2[a * fan : (a + 1) * fan, :rows] = c.astype(BF16)
        t2[a * fan : (a + 1) * fan, rows:] = s.astype(BF16)

    phase_product(coarse_2, fine_2, put_t2)

    swaps = []
    for c in range(parts):
        make_spec(c)
        contribution(c)
        if not c:
            pl.semaphore_wait(barrier, partners)
        swaps.append(swap(0, c, s_a, x_a))
        swaps[c].start()
        if c:
            swaps[c - 1].wait()
            scatter(1, c - 1, s_a, x_a, r_a)
    for side in sides:
        side.wait()
    grid_table(vis_u, du)
    swaps[-1].wait()
    scatter(1, parts - 1, s_a, x_a, r_a)
    grid_table(vis_v, dv)
    for c in range(parts):
        wait_all(1, c, r_a, half_group - 1)
        r_b[c, parity * half_group + pair] = summed(r_a, c)
        gather(2, c, r_b)

    span = M // 2 // stages
    run = n_sub * 2 * span
    lane = lanes_iota(run)
    start = lax.rem(lane // span, 2) * (M // 2) + lax.rem(lane, span)
    for s in range(n_sub):
        start = start + jnp.where(lane // (2 * span) == s, subgrid_offsets[s], 0)
    for k in range(stages):
        freqs = start + sources[k] * span if stages > 1 else start
        coarse = unit(row_start + rows_iota(rows // high, high), freqs, NIMG)
        fine = unit(rows_iota(high), freqs, NIMG)

        def put_t5(a, c, sine, at=2 * run * k):
            t5[a * high : (a + 1) * high, at : at + run] = c.astype(BF16)
            t5[a * high : (a + 1) * high, at + run : at + 2 * run] = sine.astype(BF16)

        phase_product(coarse, fine, put_t5)

    relays = []
    for c in range(parts):
        wait_all(2, c, r_b, half_group - 1)
        relays.append(relay(3, c, r_b))
        relays[c].start()

    top = M // 2

    def make_lhs(which, c):
        for g, r, k, height, width in pieces(groups, wide)[:half_group]:
            block = r_b[c, which * half_group + g]
            part = min(width, half)
            for inner in range(0, width, part):
                value = block[:, inner : inner + part]
                at = k + inner
                if at < half:
                    re = c * half + at
                    lhs[which, r : r + height, re : re + part] = value
                    lhs[which, top + r : top + r + height, M + re : M + re + part] = -value
                else:
                    im = c * half + at - half
                    lhs[which, r : r + height, M + im : M + im + part] = value
                    lhs[which, top + r : top + r + height, im : im + part] = value

    chunk = 512
    live = counts[0, 0] * BLOCK

    def model_terms(which, lanes):
        both = jnp.dot(lhs[which], du[:, lanes], preferred_element_type=F32)
        both_re, both_im = both[:top], both[top:]
        cos_v = dv[pl.ds(pl.multiple_of(which * top, top), top), lanes].astype(F32)
        sin_v = dv[pl.ds(pl.multiple_of(M + which * top, top), top), lanes].astype(F32)
        return (
            jnp.sum(cos_v * both_re + sin_v * both_im, axis=0, keepdims=True),
            jnp.sum(cos_v * both_im - sin_v * both_re, axis=0, keepdims=True),
        )

    for c in range(parts):
        make_lhs(parity, c)
    for i in range(vis // chunk):
        lanes = slice(i * chunk, (i + 1) * chunk)
        model[0:1, lanes], model[1:2, lanes] = model_terms(parity, lanes)
    for c in range(parts):
        relays[c].wait()
    for c in range(parts):
        make_lhs(1 - parity, c)
    for i in range(vis // chunk):
        lanes = slice(i * chunk, (i + 1) * chunk)
        model_re, model_im = model_terms(1 - parity, lanes)
        model_re, model_im = model_re + model[0:1, lanes], model_im + model[1:2, lanes]
        alive = lanes_iota(chunk) + i * chunk < live
        weight = weights[0:1, lanes]
        inv = F32(1.0 / M)
        res_re = jnp.where(alive, weight * (observed[0, 0:1, lanes] - model_re * inv), F32(0.0))
        res_im = jnp.where(alive, weight * (observed[0, 1:2, lanes] - model_im * inv), F32(0.0))
        residual_out[0, 0:1, lanes] = res_re
        residual_out[0, 1:2, lanes] = res_im
        r0, r1 = res_re.astype(BF16), res_im.astype(BF16)
        for c in range(parts):
            cos_u = du[c * half : (c + 1) * half, lanes]
            sin_u = du[M + c * half : M + (c + 1) * half, lanes]
            spread[c, :half, lanes] = cos_u * r0 - sin_u * r1
            spread[c, half:, lanes] = sin_u * r0 + cos_u * r1

    across = (((1,), (1,)), ((), ()))
    swaps = []
    for c in range(parts):
        for i in range(2):
            here = slice(i * M, (i + 1) * M)
            acc[here, :] = lax.dot_general(
                dv[here, :], spread[c], across, preferred_element_type=F32
            )
        acc[:M, :half] = acc[:M, :half] - acc[M:, half:]
        acc[:M, half:] = acc[:M, half:] + acc[M:, :half]
        split(c, s_c, F32((vis * groups) ** (-0.5)))
        swaps.append(swap(4, c, s_c, x_c))
        swaps[c].start()
        if c:
            swaps[c - 1].wait()
            scatter(5, c - 1, s_c, x_c, r_c)

    out_cols = sub * local_cols + lanes_iota(local_cols)
    coarse = unit(column_offset[0] + rows_iota(M // step, step), out_cols, NIMG)
    fine = unit(rows_iota(step), out_cols, NIMG)
    out_norm = F32(M ** (-0.5))

    def put_t6(a, c, s):
        which, at = a * step // half, a * step % half
        t6[which, at : at + step, :] = (c * out_norm).astype(BF16)
        t6[which, half + at : half + at + step, :] = (s * -out_norm).astype(BF16)

    phase_product(coarse, fine, put_t6)
    swaps[-1].wait()
    scatter(5, parts - 1, s_c, x_c, r_c)

    def slab(c, f, count):
        return r_d.at[c, pl.ds(d_slot(parity, f, 0), count)]

    def column_copy(c, k, f, device, arrived):
        piece = r_d.at[c, d_slot(parity, f, spot)]
        return pltpu.make_async_remote_copy(
            piece, piece, d_send.at[0, c, k], d_recv.at[0, c, arrived], device, MESH
        )

    def level_copy(c, f, piece, device):
        return pltpu.make_async_remote_copy(
            piece, piece, d_send.at[1, c, f], d_recv.at[1, c, f], device, MESH
        )

    def level_sends(c, f):
        for device in levels:
            level_copy(c, f, r_d.at[c, d_slot(parity, f, spot)], device).start()

    def level_done(c, f):
        return level_copy(c, f, slab(c, f, plane - 1), sibling)

    def level_relay(c, f):
        whole = slab(c, f, plane)
        return pltpu.make_async_remote_copy(
            whole, whole, d_send.at[2, c, f], d_recv.at[2, c, f], sibling, MESH
        )

    for c in range(parts):
        wait_all(5, c, r_c, half_group - 1)
        r_d[c, d_slot(parity, facet, spot)] = summed(r_c, c)
        for k in range(n_facet - 1, 0, -1):
            device = {"facet": sources[k], "sub": sub, "base": base}
            column_copy(c, k, facet, device, facet).start()
        level_sends(c, facet)
    scale = F32((n_sub * M) ** (-0.5))

    def pass_on(c):
        for k in range(1, n_facet):
            column_copy(c, k, sources[k], sibling, sources[k]).wait_recv()
            level_sends(c, sources[k])

    def land(c, k):
        for f in [sources[k]] if stages > 1 else sources:
            level_done(c, f).wait_recv()
            level_relay(c, f).start()

    def build(c, k):
        for f in [sources[k]] if stages > 1 else sources:
            level_relay(c, f).wait_recv()
        for g, r, col, height, width in pieces(groups, wide)[:half_group]:
            if stages > 1:
                if g >= pairs:
                    continue
                f = sources[k]
            else:
                f = g // pairs
            part = min(width, half)
            for s in range(n_sub):
                for which in range(2):
                    block = r_d[c, d_slot(which, f, s * pairs + g % pairs)]
                    at = 2 * run * k + (2 * s + which) * span + r
                    low = slice(at + run, at + run + height)
                    for inner in range(0, width, part):
                        value = block[:, inner : inner + part]
                        to = col + inner
                        zed[c, at : at + height, to : to + part] = value
                        if to < half:
                            zed[c, low, half + to : half + to + part] = value
                        else:
                            zed[c, low, to - half : to - half + part] = -value

    def take(c, k):
        build(c, k)
        some = slice(2 * run * k, 2 * run * (k + 1))
        for i in range(rows // tile):
            here = slice(i * tile, (i + 1) * tile)
            term = jnp.dot(t5[here, some], zed[c, some], preferred_element_type=F32)
            wave[c, here, :] = wave[c, here, :] + term if k else term

    def finish(c):
        take(c, stages - 1)
        for i in range(rows // tile):
            here = slice(i * tile, (i + 1) * tile)
            share[here, :] = (wave[c, here, :] * scale).astype(BF16)
        for i in range(rows // tile):
            here = slice(i * tile, (i + 1) * tile)
            term = jnp.dot(share[here, :], t6[c], preferred_element_type=F32)
            partial[here, :] = partial[here, :] + term if c else term

    pass_on(0)
    inner = range(1, stages - 1)
    if parts == 2 and stages > 1:
        land(0, 0)
        pass_on(1)
        land(1, 0)
        for k in inner:
            land(0, k)
        take(0, 0)
        take(1, 0)
        land(0, stages - 1)
        for k in inner:
            land(1, k)
        for k in inner:
            take(0, k)
        land(1, stages - 1)
        for k in inner:
            take(1, k)
        finish(0)
        build(1, stages - 1)
    else:
        for c in range(1, parts):
            pass_on(c)
        for c in range(parts):
            for k in range(stages):
                land(c, k)
        for c in range(parts):
            for k in range(stages - 1):
                take(c, k)
            if c + 1 < parts:
                finish(c)
        build(parts - 1, stages - 1)

    for c in range(parts):
        for k in range(n_facet):
            level_done(c, sources[k]).wait_send()
            level_relay(c, sources[k]).wait_send()
            if k:
                column_copy(c, k, facet, sibling, facet).wait_send()


def deliver(
    scale,
    stages,
    residual,
    t5,
    t6,
    zed,
    partial,
    wave,
    residual_out,
    update_out,
    share,
    update,
    sem,
    sems,
):
    first = pltpu.make_async_copy(residual, residual_out, sem)
    first.start()
    rows, depth = t5.shape
    tile = min(512, rows)
    last = zed.shape[0] - 1
    some = slice(depth - depth // stages, depth)
    tiles = [slice(i * tile, (i + 1) * tile) for i in range(rows // tile)]
    writes = []
    for start in range(0, len(tiles), 2):
        for here in tiles[start : start + 2]:
            total = jnp.dot(t5[here, some], zed[last, some], preferred_element_type=F32)
            if stages > 1:
                total = wave[last, here, :] + total
            share[here, :] = (total * F32(scale)).astype(BF16)
        for i, here in list(enumerate(tiles))[start : start + 2]:
            term = jnp.dot(share[here, :], t6[last], preferred_element_type=F32)
            if last:
                term = partial[here, :] + term
            update[here, :] = term.astype(BF16)
            writes.append(
                pltpu.make_async_copy(update.at[here, :], update_out.at[here, :], sems.at[i])
            )
            writes[i].start()
    first.wait()
    for write in writes:
        write.wait()


def shards(
    sizes,
    sky_image,
    facet_rows,
    column_offset,
    subgrid_offsets,
    vis_u,
    vis_v,
    observed,
    weights,
    block_counts,
):
    n_facet, n_sub, n_base = sizes
    groups = n_facet * n_base
    parts = halves(groups)
    wide = 2 * M // parts
    rows, columns = sky_image.shape
    vis = vis_u.shape[1]
    local_cols = columns // n_sub
    _, _, _, height, width = pieces(groups, wide)[0]
    smem = pl.BlockSpec(memory_space=pltpu.SMEM)
    vmem = pl.BlockSpec(memory_space=pltpu.VMEM)
    hbm = pl.BlockSpec(memory_space=pltpu.HBM)
    block = (parts, groups, height, width)
    half_block = (parts, groups // 2, height, width)
    kept = (
        pltpu.VMEM((rows, 2 * M * n_sub), BF16),
        pltpu.VMEM((parts, wide, local_cols), BF16),
        pltpu.VMEM((parts, 2 * M * n_sub, wide), BF16),
        pltpu.VMEM((rows, local_cols), F32),
        pltpu.VMEM((parts, rows, wide), F32),
    )
    room = sum(math.prod(k.shape) * jnp.dtype(k.dtype).itemsize for k in kept)
    results = pl.pallas_call(
        functools.partial(kernel, sizes),
        out_shape=(
            pltpu.VMEM(observed.shape, F32),
            *kept,
        ),
        in_specs=[hbm, smem, hbm, smem] + [hbm] * 5,
        out_specs=(vmem,) * 6,
        scratch_shapes=[
            pltpu.SMEM(facet_rows.shape, jnp.int32),
            pltpu.SMEM(subgrid_offsets.shape, jnp.int32),
            pltpu.VMEM((rows, columns), BF16),
            pltpu.VMEM(vis_u.shape, jnp.int32),
            pltpu.VMEM(vis_v.shape, jnp.int32),
            pltpu.VMEM(observed.shape, F32),
            pltpu.VMEM(weights.shape, F32),
            pltpu.VMEM((parts, columns, wide), BF16),
            pltpu.VMEM((parts, 2 * rows, wide), BF16),
            pltpu.VMEM((M, 2 * rows), BF16),
            pltpu.VMEM((2 * M, vis), BF16),
            pltpu.VMEM((2 * M, vis), BF16),
            pltpu.VMEM((2, M, 2 * M), BF16),
            pltpu.VMEM((2, vis), F32),
            pltpu.VMEM((2 * M, wide), F32),
            pltpu.VMEM((parts, wide, vis), BF16),
            pltpu.VMEM((rows, wide), BF16),
            pltpu.VMEM(block, BF16),
            pltpu.VMEM(half_block, BF16),
            pltpu.VMEM(half_block, BF16),
            pltpu.VMEM(block, BF16),
            pltpu.VMEM(block, BF16),
            pltpu.VMEM(half_block, BF16),
            pltpu.VMEM(half_block, BF16),
            pltpu.VMEM((parts, n_sub * groups, height, width), BF16),
            pltpu.SemaphoreType.DMA((rows // min(256, rows),)),
            pltpu.SemaphoreType.DMA((4,)),
            pltpu.SemaphoreType.DMA((2,)),
            pltpu.SemaphoreType.DMA((6, parts)),
            pltpu.SemaphoreType.DMA((6, parts)),
            pltpu.SemaphoreType.DMA((3, parts, n_facet)),
            pltpu.SemaphoreType.DMA((3, parts, n_facet)),
        ],
        compiler_params=pltpu.CompilerParams(
            collective_id=0, has_side_effects=True, vmem_limit_bytes=61 * 1024 * 1024 - room
        ),
        name="column",
    )(
        facet_rows,
        column_offset,
        subgrid_offsets,
        block_counts,
        sky_image,
        vis_u,
        vis_v,
        observed,
        weights,
    )
    return pl.pallas_call(
        functools.partial(deliver, (n_sub * M) ** (-0.5), layers(n_facet, groups)),
        out_shape=(
            jax.ShapeDtypeStruct(observed.shape, F32),
            jax.ShapeDtypeStruct((rows, local_cols), BF16),
        ),
        in_specs=[vmem] * 6,
        out_specs=(hbm, hbm),
        scratch_shapes=[
            pltpu.VMEM((rows, wide), BF16),
            pltpu.VMEM((rows, local_cols), BF16),
            pltpu.SemaphoreType.DMA,
            pltpu.SemaphoreType.DMA((rows // min(512, rows),)),
        ],
        compiler_params=pltpu.CompilerParams(vmem_limit_bytes=8 * 1024 * 1024),
        name="deliver",
    )(*[pltpu.with_memory_space_constraint(r, pltpu.VMEM) for r in results])


def solution(mesh):
    sizes = (mesh.shape["facet"], mesh.shape["sub"], mesh.shape["base"])
    return jax.shard_map(
        functools.partial(shards, sizes),
        mesh=mesh,
        in_specs=(
            P(("facet", "base"), None),
            P(),
            P(),
            P(),
            P("sub", ("facet", "base")),
            P("sub", ("facet", "base")),
            P("sub", None, ("facet", "base")),
            P("sub", ("facet", "base")),
            P("sub", ("facet", "base")),
        ),
        out_specs=(P("sub", None, ("facet", "base")), P(("facet", "base"), "sub")),
        check_vma=False,
    )
```
